32 devices in a mesh: dp: 8 (over z, x), mp: 4 (over y, core).
Axes of the slice: x: 2, y: 2, z: 4, core: 2. Of those that a mesh axis runs over, the one named last changes fastest.
Arguments:
- tokens: bfloat16 [2048, 2048], P('dp'), may hold values from -6 to 6
- targets: bfloat16 [2048, 2048], P('dp'), may hold values from -6 to 6
- loss_weights: float32 [2048], P('dp'), may hold values from 0.4 to 14, as said below
- segments: int32 [8, 256], P('dp'), may hold values from 0 to 3, never falling along the last dimension, each value on 1 to 128 neighbouring positions
- probe_model: int32 [8, 2048], P('dp'), may hold values from 0 to 1
- probe_heads: int32 [8, 2, 2048], P('dp', None, 'mp'), may hold values from 0 to 1
- norm_gain: float32 [2048], replicated, may hold values from 0.5 to 1.5
- w_query: bfloat16 [2048, 2048], P(None, 'mp'), may hold values from -0.125 to 0.125
- w_key: bfloat16 [2048, 2048], P(None, 'mp'), may hold values from -0.125 to 0.125
- w_value: bfloat16 [2048, 2048], P(None, 'mp'), may hold values from -0.125 to 0.125
- w_out: bfloat16 [2048, 2048], P('mp'), may hold values from -0.125 to 0.125
Outputs:
- diag_query: float32 [2048, 2048], P('dp', 'mp')
- diag_key: float32 [2048, 2048], P('dp', 'mp')
- mean_diag: float32 [2], replicated
The draws below stay inside these ranges and needn't reach their ends.
Inputs may be any that keep to these rules, and one draw needn't show every extreme that they name: `segments`: the documents of a sequence are runs of 1 to 128 tokens, numbered upwards from 0. `loss_weights`: positive weights.
All inputs are finite; a program needn't handle non-finite values.
Results may differ from the reference program's by a relative error of at most 0.0099.
Values may be sent and summed in bfloat16 or wider, within the bound.
A program may use at most 128 MiB of HBM per device.

```python
import math
import jax
import jax.numpy as jnp
import numpy as np
from jax import lax

D = 2048
HEAD_DIM = 128
SEQ = 256
DOCS = 4
GROUPS = 8
TOKENS = 2048
FEAT = 2048


def draw_loss_weights(key, part):
    group_index = (jnp.arange(TOKENS, dtype=jnp.int32) // SEQ).astype(jnp.float32)
    rising = 1.0 + 2.0 * group_index / max(GROUPS - 1, 1)
    base_values = jnp.exp(jax.random.uniform(key, (TOKENS,), jnp.float32, jnp.log(0.5), jnp.log(2.0)))
    return (rising * base_values).astype(jnp.float32)


def plant(values, key, least, largest):
    place = [jax.random.randint(jax.random.fold_in(key, axis), (), 0, length) for axis, length in enumerate(values.shape)]
    widest = values.shape.index(max(values.shape))
    next_to = place[:widest] + [(place[widest] + 1) % values.shape[widest]] + place[widest + 1:]
    return values.at[tuple(place)].set(least).at[tuple(next_to)].set(largest)


def with_spikes(array, stream_key, source, target, blocks, factor):
    owner, partner = [(jnp.arange(array.shape[axis_at]) // (array.shape[axis_at] // blocks)).reshape([-1 if axis == axis_at else 1 for axis in range(array.ndim)]) for axis_at in (source, target)]
    chosen = jax.random.permutation(stream_key, blocks)[partner]
    strong = (owner == chosen) | (owner == (partner + blocks // 2) % blocks)
    return jnp.where(strong, factor * array, array)


def block_scale(stream_key, dims, shards, low, top_value):
    level, own = 1.0, jax.random.fold_in(stream_key, 6)
    for dim, blocks in shards:
        steps = jnp.exp(jax.random.uniform(jax.random.fold_in(own, dim), (blocks,), jnp.float32, low / len(shards), top_value / len(shards)))
        level = level * jnp.repeat(steps, dims[dim] // blocks).reshape([-1 if axis == dim else 1 for axis in range(len(dims))])
    return level


def profile(count, total, reach, skew):
    loads = [(1 << 20) // math.isqrt(standing ** skew) + 1 for standing in range(2, count + 1)]
    surplus, given = total - reach - (count - 1), [1] * (count - 1)
    while surplus > 0:
        movable = [i for i in range(count - 1) if given[i] < reach]
        whole, left = sum([loads[i] for i in movable]), surplus
        for i in movable:
            extra = min(reach - given[i], max(1, left * loads[i] // whole), surplus)
            given[i] = given[i] + extra
            surplus = surplus - extra
    return np.array([reach] + given)


def ragged_sizes(rng, amount, total, most, slope):
    if amount == 2:
        one = jax.random.randint(rng, (), max(1, total - most), min(most, total - 1) + 1)
        return jnp.stack([one, total - one])
    sizes = jnp.asarray(profile(amount, total, most, slope), jnp.int32)
    twos = (amount - 1) // 2
    source_of, sink = sizes[1:1 + 2 * twos:2], sizes[2:2 + 2 * twos:2]
    slack = jnp.minimum(source_of - 1, most - sink)
    moved = jax.random.randint(jax.random.fold_in(rng, 1), (twos,), 0, 1 << 20) % (slack + 1)
    sizes = sizes.at[1:1 + 2 * twos:2].set(source_of - moved).at[2:2 + 2 * twos:2].set(sink + moved)
    return sizes[jax.random.permutation(jax.random.fold_in(rng, 2), amount)]


def gaussian(key, dims, spread, most, split=(), kind=jnp.bfloat16):
    gain = block_scale(key, dims, split, -0.22, 0.18) if split else 1.0
    values = jax.random.normal(key, dims, jnp.float32) * spread * gain
    return jnp.minimum(jnp.maximum(values, -most), most).astype(kind)


def heavy_noise(key, shape, scale, limit, pieces, heavy, kind=jnp.bfloat16):
    values = scale * jax.random.normal(key, shape, jnp.float32)
    if pieces:
        values = values * block_scale(key, shape, pieces, -0.22, 0.18)
    return jnp.clip(with_spikes(values, jax.random.fold_in(key, 3), *heavy), -limit, limit).astype(kind)


def setup_inputs(seed: int = 0) -> dict:
    seeds = jax.random.split(jax.random.key(seed), 12)
    tokens = heavy_noise(seeds[0], (TOKENS, D), 1.0, 6.0, ((0, 8),), (0, 1, 8, 2.0))
    targets = heavy_noise(seeds[1], (TOKENS, D), 1.0, 6.0, ((0, 8),), (0, 1, 8, 2.0))
    loss_weights = draw_loss_weights(jax.random.fold_in(seeds[11], 71), 0)
    segments = jax.vmap(lambda own: jnp.searchsorted(jnp.cumsum(ragged_sizes(own, DOCS, SEQ, SEQ // 2, 0)), jnp.arange(SEQ), side="right"))(jax.random.split(seeds[3], GROUPS)).reshape((GROUPS, SEQ)).astype(jnp.int32)
    probe_model = plant(jax.random.randint(seeds[4], (GROUPS, D), 0, 2), jax.random.fold_in(seeds[4], 1), 0, 1).astype(jnp.int32)
    probe_heads = plant(jax.random.randint(seeds[5], (GROUPS, 2, FEAT), 0, 2), jax.random.fold_in(seeds[5], 1), 0, 1).astype(jnp.int32)
    norm_gain = jnp.clip(1.0 + 0.1 * jax.random.normal(seeds[6], (D,), jnp.float32), 0.5, 1.5)
    w_query = gaussian(seeds[7], (D, FEAT), D ** -0.5, 0.125, ((1, 4),))
    w_key = gaussian(seeds[8], (D, FEAT), D ** -0.5, 0.125, ((1, 4),))
    w_value = gaussian(seeds[9], (D, FEAT), D ** -0.5, 0.125, ((1, 4),))
    w_out = gaussian(seeds[10], (FEAT, D), FEAT ** -0.5, 0.125, ((0, 4),))
    return dict(tokens=tokens, targets=targets, loss_weights=loss_weights, segments=segments, probe_model=probe_model, probe_heads=probe_heads, norm_gain=norm_gain, w_query=w_query, w_key=w_key, w_value=w_value, w_out=w_out)


exact_mode = lax.Precision.HIGHEST
norm_epsilon = 1e-06

def sign_pattern(row_index, col_index):
    mixed_index = (row_index[:, None] * 1103 + col_index[None, :] * 2713 + 7) % 32749
    mixed_index = mixed_index * mixed_index % 32749
    return 1.0 - 2.0 * (mixed_index // 5 % 2).astype(jnp.float32)

def rope_tables(length):
    position = jnp.arange(length, dtype=jnp.int32).astype(jnp.float32)
    exponent = jnp.arange(0, HEAD_DIM, 2, dtype=jnp.int32).astype(jnp.float32) / HEAD_DIM
    frequency = 10000.0 ** (-exponent)
    angles = position[:, None] * frequency[None, :]
    return (jnp.cos(angles)[:, None, :], jnp.sin(angles)[:, None, :])

def rotate(packed, cosine, sine_table):
    half_dim = packed.shape[-1] // 2
    front_half = packed[..., :half_dim]
    back_half = packed[..., half_dim:]
    return jnp.concatenate([front_half * cosine - back_half * sine_table, back_half * cosine + front_half * sine_table], axis=-1)

def attend(query, keys, values, doc_ids):
    length = query.shape[0]
    head_count = query.shape[1] // HEAD_DIM
    cosine, sine_table = rope_tables(length)
    rotated_query = rotate(query.reshape(length, head_count, HEAD_DIM), cosine, sine_table)
    rotated_keys = rotate(keys.reshape(length, head_count, HEAD_DIM), cosine, sine_table)
    scores = jnp.einsum('qhd,khd->hqk', rotated_query, rotated_keys, precision=exact_mode) * HEAD_DIM ** (-0.5)
    position = jnp.arange(length, dtype=jnp.int32)
    allowed = (position[:, None] >= position[None, :]) & (doc_ids[:, None] == doc_ids[None, :])
    raised = jnp.where(allowed[None], jnp.exp(scores), 0.0)
    attention_weights = raised / lax.optimization_barrier(jnp.sum(raised, axis=-1, keepdims=True))
    mixed_values = jnp.einsum('hqk,khd->qhd', attention_weights, values.reshape(length, head_count, HEAD_DIM), precision=exact_mode)
    return mixed_values.reshape(length, head_count * HEAD_DIM)

def tangent_of(query, keys, values, doc_ids, tangents):

    def forward(query_in, keys_in, values_in):
        return attend(query_in, keys_in, values_in, doc_ids)
    result, pullback = jax.vjp(forward, query, keys, values)

    def pulled(cotangent):
        return pullback(cotangent)
    unused, pushforward = jax.vjp(pulled, jnp.zeros_like(result))
    return (result, pushforward((tangents[0], tangents[1], jnp.zeros_like(values)))[0])

def second_order(query, keys, values, doc_ids, back_grad, tangents, back_tangent):

    def inner(query_in, keys_in):

        def paired(query_at, keys_at):
            return jnp.sum(attend(query_at, keys_at, values, doc_ids) * back_grad)
        gradients = jax.grad(paired, argnums=(0, 1))(query_in, keys_in)
        summed = jnp.sum(gradients[0] * tangents[0]) + jnp.sum(gradients[1] * tangents[1])
        return summed + jnp.sum(attend(query_in, keys_in, values, doc_ids) * back_tangent)
    return jax.grad(inner, argnums=(0, 1))(query, keys)

def bf_dot(left, right):
    return jnp.dot(left, right, preferred_element_type=jnp.float32)

def reference(tokens, targets, loss_weights, segments, probe_model, probe_heads, norm_gain, w_query, w_key, w_value, w_out):
    pattern = sign_pattern(jnp.arange(D, dtype=jnp.int32), jnp.arange(FEAT, dtype=jnp.int32))

    def group_step(carry, inputs):
        group_tokens, group_targets, group_weights, doc_ids, model_bits, head_bits = inputs
        model_sign = 2.0 * model_bits.astype(jnp.float32) - 1.0
        head_sign = 2.0 * head_bits.astype(jnp.float32) - 1.0
        probe_query = (model_sign[:, None] * head_sign[0][None, :] * pattern).astype(jnp.bfloat16)
        probe_key = (model_sign[:, None] * head_sign[1][None, :] * pattern).astype(jnp.bfloat16)
        token_float = group_tokens.astype(jnp.float32)
        inverse_rms = lax.rsqrt(lax.optimization_barrier(jnp.mean(token_float * token_float, axis=1, keepdims=True)) + norm_epsilon)
        normed = (token_float * inverse_rms * norm_gain).astype(jnp.bfloat16)
        query = bf_dot(normed, w_query)
        keys = bf_dot(normed, w_key)
        values = bf_dot(normed, w_value)
        d_query = bf_dot(normed, probe_query)
        d_keys = bf_dot(normed, probe_key)
        attended_full, d_attended_full = tangent_of(query, keys, values, doc_ids, (d_query, d_keys))
        attended = attended_full.astype(jnp.bfloat16)
        d_attended = d_attended_full.astype(jnp.bfloat16)
        weight_rows = group_weights / SEQ
        output = token_float + bf_dot(attended, w_out)
        residual = ((output - group_targets.astype(jnp.float32)) * weight_rows[:, None]).astype(jnp.bfloat16)
        d_output = bf_dot(d_attended, w_out)
        d_residual = (d_output * weight_rows[:, None]).astype(jnp.bfloat16)
        back_grad = bf_dot(residual, w_out.T)
        back_tangent = bf_dot(d_residual, w_out.T)
        h_query, h_keys = second_order(query, keys, values, doc_ids, back_grad, (d_query, d_keys), back_tangent)
        est_query = probe_query.astype(jnp.float32) * bf_dot(normed.T, h_query.astype(jnp.bfloat16))
        est_key = probe_key.astype(jnp.float32) * bf_dot(normed.T, h_keys.astype(jnp.bfloat16))
        return ((carry[0] + est_query, carry[1] + est_key), None)
    zero_feat = jnp.zeros((D, FEAT), jnp.float32)
    inputs = (tokens.reshape(GROUPS, SEQ, D), targets.reshape(GROUPS, SEQ, D), loss_weights.reshape(GROUPS, SEQ), segments, probe_model, probe_heads)
    sums, unused = lax.scan(group_step, (zero_feat, zero_feat), inputs)
    diag_query = sums[0] / GROUPS
    diag_key = sums[1] / GROUPS
    mean_diag = jnp.stack([jnp.sum(diag_query), jnp.sum(diag_key)]) / (D * FEAT)
    return (diag_query, diag_key, mean_diag)
```

```python
import functools

import jax
import jax.numpy as jnp
import numpy as np
from jax import lax
from jax.experimental import pallas as pl
from jax.experimental.pallas import tpu as pltpu
from jax.sharding import PartitionSpec as P

HEAD_DIM = 128
PAIR = 2 * HEAD_DIM
PRIME = 32749
F32 = jnp.float32
BF16 = jnp.bfloat16
MESH = pl.DeviceIdType.MESH

NN = (((1,), (0,)), ((), ()))
NT = (((1,), (1,)), ((), ()))
TN = (((0,), (0,)), ((), ()))


def dot(left, right, dims=NN):
    return lax.dot_general(left, right, dims, preferred_element_type=F32)


def low(left, right, dims=NN):
    return dot(left.astype(BF16), right.astype(BF16), dims)


def halves(array):
    high = array.astype(BF16)
    return high, (array - high.astype(F32)).astype(BF16)


def residue(whole):
    value = whole.astype(F32)
    left = value - jnp.floor(value * (1.0 / PRIME)) * PRIME
    left = jnp.where(left < 0, left + PRIME, left)
    left = jnp.where(left >= PRIME, left - PRIME, left)
    return left.astype(jnp.int32)


def pattern_block(row_part, col_part):
    mixed = row_part + col_part
    mixed = jnp.where(mixed >= PRIME, mixed - PRIME, mixed)
    square = mixed * mixed
    times = (square.astype(F32) * (1.0 / PRIME)).astype(jnp.int32)
    left = square - times * PRIME
    left = jnp.where(left < 0, left + PRIME, left)
    left = jnp.where(left >= PRIME, left - PRIME, left)
    odd = jnp.bitwise_and(jnp.right_shift(left * 52429, 18), 1)
    return jnp.where(odd == 1, -1.0, 1.0).astype(BF16)


def rotate(array, cos, sin):
    return array * cos + pltpu.roll(array, HEAD_DIM // 2, 1) * sin


def unrotate(array, cos, sin):
    return array * cos - pltpu.roll(array, HEAD_DIM // 2, 1) * sin


def kernel(
    groups,
    parts,
    entries,
    chunks,
    weights_row,
    seg_row,
    model_bits,
    head_bits,
    gain,
    cosine,
    sine,
    tokens_hbm,
    targets_hbm,
    wq_hbm,
    wk_hbm,
    wv_hbm,
    wo_hbm,
    diag_query,
    diag_key,
    mean_out,
    tokens,
    targets,
    wq,
    wk,
    wv,
    wo,
    wo_turned,
    normed,
    signed,
    slabs,
    slabs_turned,
    pattern,
    product,
    left_main,
    left_rest,
    right_main,
    right_rest,
    values,
    soft,
    d_soft,
    attended,
    out_send,
    own_part,
    pair_recv,
    chip_send,
    chip_recv,
    residual,
    hk_sum,
    gathered,
    x_send,
    x_recv,
    own_sum,
    result,
    stat_send,
    stat_recv,
    stat_all,
    load_sem,
    slab_ssem,
    slab_rsem,
    share_ssem,
    share_rsem,
    pair_ssem,
    pair_rsem,
    chip_ssem,
    chip_rsem,
    res_ssem,
    res_rsem,
    line_ssem,
    line_rsem,
    x_ssem,
    x_rsem,
    stat_ssem,
    stat_rsem,
    all_ssem,
    all_rsem,
    out_sem,
):
    seq, width = tokens.shape
    feat = wq.shape[1]
    heads = feat // HEAD_DIM
    block = width // groups
    lines = groups // 2
    slab = 2 * block
    half = seq // 2
    count = len(chunks)
    dp = lax.axis_index("dp")
    mp = lax.axis_index("mp")
    kind = lax.rem(mp, 2)
    other = 1 - kind
    pair = mp + 1 - 2 * kind
    chip = lax.rem(mp + 2, parts)
    inner = lax.rem(dp, 2)
    outer = dp // 2
    x_peer = dp + 1 - 2 * inner

    loads = []
    for n, (source, target) in enumerate(
        (
            (tokens_hbm, tokens),
            (wq_hbm, wq),
            (wk_hbm, wk),
            (wv_hbm, wv),
            (wo_hbm, wo),
            (targets_hbm, targets),
        )
    ):
        load = pltpu.make_async_copy(source, target, load_sem.at[n])
        load.start()
        loads.append(load)

    barrier = pltpu.get_barrier_semaphore()
    for step in range(1, lines):
        peer = lax.rem(outer + step, lines) * 2 + inner
        pl.semaphore_signal(barrier, inc=1, device_id={"dp": peer}, device_id_type=MESH)
    pl.semaphore_signal(barrier, inc=1, device_id={"dp": x_peer}, device_id_type=MESH)
    pl.semaphore_signal(barrier, inc=1, device_id={"mp": pair}, device_id_type=MESH)
    pl.semaphore_signal(barrier, inc=1, device_id={"mp": chip}, device_id_type=MESH)

    col_part = residue((mp * feat + lax.broadcasted_iota(jnp.int32, (1, feat), 1)) * 2713)
    for start in range(0, width, 256):
        row_part = residue((start + lax.broadcasted_iota(jnp.int32, (256, 1), 0)) * 1103 + 7)
        pattern[start : start + 256, :] = pattern_block(row_part, col_part)

    model_sign = 2.0 * model_bits[...].astype(F32) - 1.0
    head_sign = 2.0 * head_bits[0].astype(F32) - 1.0
    loads[0].wait()
    token_float = tokens[...].astype(F32)
    inverse = lax.rsqrt(jnp.sum(token_float * token_float, axis=1, keepdims=True) / width + 1e-06)
    for start in range(0, width, 256):
        cols = slice(start, start + 256)
        part = (tokens[:, cols].astype(F32) * inverse * gain[:, cols]).astype(BF16)
        normed[:, cols] = part
        signed[:, cols] = (part.astype(F32) * model_sign[:, cols]).astype(BF16)

    pl.semaphore_wait(barrier, lines + 2)

    def slab_copy(step):
        peer = lax.rem(outer + step, lines)
        return pltpu.make_async_remote_copy(
            src_ref=signed.at[
                pl.ds(pl.multiple_of(kind * half, half), half),
                pl.ds(pl.multiple_of(peer * slab, slab), slab),
            ],
            dst_ref=slabs.at[outer, pl.ds(pl.multiple_of(kind * half, half), half), :],
            send_sem=slab_ssem.at[step],
            recv_sem=slab_rsem.at[step],
            device_id={"dp": peer * 2 + inner},
            device_id_type=MESH,
        )

    def share_copy(step):
        owner = lax.rem(outer - step + lines, lines)
        mine = slabs.at[owner, pl.ds(pl.multiple_of(kind * half, half), half), :]
        return pltpu.make_async_remote_copy(
            src_ref=mine,
            dst_ref=mine,
            send_sem=share_ssem.at[step],
            recv_sem=share_rsem.at[step],
            device_id={"mp": pair},
            device_id_type=MESH,
        )

    for step in range(1, lines):
        slab_copy(step).start()

    cos = cosine[...]
    sin = sine[...]
    scale = HEAD_DIM ** (-0.5)

    loads[1].wait()
    query = dot(normed[...], wq[...])
    for h in range(heads):
        cols = slice(h * HEAD_DIM, (h + 1) * HEAD_DIM)
        high, rest = halves(rotate(query[:, cols], cos, sin))
        left_main[h, :, HEAD_DIM:] = high
        left_rest[h, :, HEAD_DIM:] = rest
    loads[2].wait()
    keys = dot(normed[...], wk[...])
    for h in range(heads):
        cols = slice(h * HEAD_DIM, (h + 1) * HEAD_DIM)
        high, rest = halves(rotate(keys[:, cols], cos, sin))
        right_main[h, :, :HEAD_DIM] = high
        right_rest[h, :, :HEAD_DIM] = rest
    product[...] = dot(signed[...], pattern[...])
    for h in range(heads):
        cols = slice(h * HEAD_DIM, (h + 1) * HEAD_DIM)
        probe = product[:, cols]
        high, rest = halves(rotate(probe * head_sign[0:1, cols], cos, sin))
        left_main[h, :, :HEAD_DIM] = high
        left_rest[h, :, :HEAD_DIM] = rest
        high, rest = halves(rotate(probe * head_sign[1:2, cols], cos, sin))
        right_main[h, :, HEAD_DIM:] = high
        right_rest[h, :, HEAD_DIM:] = rest
    loads[3].wait()
    values[...] = dot(normed[...], wv[...]).astype(BF16)

    place_q = lax.broadcasted_iota(jnp.int32, (seq, seq), 0)
    place_k = lax.broadcasted_iota(jnp.int32, (seq, seq), 1)
    same = place_q == place_k
    segments = seg_row[...].astype(F32)
    seg_col = jnp.sum(jnp.where(same, segments, 0.0), axis=1, keepdims=True)
    row_weights = jnp.sum(jnp.where(same, weights_row[...], 0.0), axis=1, keepdims=True) / seq

    def pair_copy(c):
        first, rows = chunks[c]
        return pltpu.make_async_remote_copy(
            src_ref=out_send.at[pl.ds(first, rows), :],
            dst_ref=pair_recv.at[pl.ds(first, rows), :],
            send_sem=pair_ssem.at[c],
            recv_sem=pair_rsem.at[c],
            device_id={"mp": pair},
            device_id_type=MESH,
        )

    def chip_copy(c):
        first, rows = chunks[c]
        return pltpu.make_async_remote_copy(
            src_ref=chip_send.at[pl.ds(first, rows), :],
            dst_ref=chip_recv.at[pl.ds(first, rows), :],
            send_sem=chip_ssem.at[c],
            recv_sem=chip_rsem.at[c],
            device_id={"mp": chip},
            device_id_type=MESH,
        )

    def res_copy(c, which):
        first, rows = chunks[c]
        return pltpu.make_async_remote_copy(
            src_ref=residual.at[which, pl.ds(first, rows), :],
            dst_ref=residual.at[which, pl.ds(first, rows), :],
            send_sem=res_ssem.at[c],
            recv_sem=res_rsem.at[c],
            device_id={"mp": pair},
            device_id_type=MESH,
        )

    def attend(c):
        first, rows = chunks[c]
        reach = first + rows
        span = slice(first, reach)
        allowed = (
            (first + lax.broadcasted_iota(jnp.int32, (rows, reach), 0))
            >= lax.broadcasted_iota(jnp.int32, (rows, reach), 1)
        ) & (seg_col[span, :] == segments[:, :reach])
        for h in range(heads):
            cols = slice(h * HEAD_DIM, (h + 1) * HEAD_DIM)
            both = left_main[h, span, :]
            rest = left_rest[h, span, :]
            main_k = right_main[h, :reach, :]
            rest_k = right_rest[h, :reach, :]
            q = both[:, HEAD_DIM:]
            k = main_k[:, :HEAD_DIM]
            scores = (
                dot(q, k, NT)
                + dot(rest[:, HEAD_DIM:], k, NT)
                + dot(q, rest_k[:, :HEAD_DIM], NT)
            ) * scale
            d_scores = (dot(both, main_k, NT) + dot(rest, main_k, NT) + dot(both, rest_k, NT)) * scale
            raised = jnp.where(allowed, jnp.exp(scores), 0.0)
            p = raised / jnp.sum(raised, axis=1, keepdims=True)
            d_p = p * (d_scores - jnp.sum(p * d_scores, axis=1, keepdims=True))
            soft[h, span, :reach] = p
            d_soft[h, span, :reach] = d_p
            v = values[:reach, cols]
            attended[0, span, cols] = low(p, v).astype(BF16)
            attended[1, span, cols] = low(d_p, v).astype(BF16)

    def project(c):
        first, rows = chunks[c]
        span = slice(first, first + rows)
        out_send[span, :] = dot(attended[other, span, :], wo[...]).astype(BF16)
        pair_copy(c).start()
        own_part[span, :] = dot(attended[kind, span, :], wo[...])
        pair_copy(c).wait_recv()
        summed = own_part[span, :] + pair_recv[span, :].astype(F32)
        own_part[span, :] = summed
        chip_send[span, :] = summed.astype(BF16)
        chip_copy(c).start()

    def line_copy(c, h, slot, target, way):
        first, rows = chunks[c]
        here = gathered.at[h, slot, pl.ds(first, rows), :]
        return pltpu.make_async_remote_copy(
            src_ref=here,
            dst_ref=here,
            send_sem=line_ssem.at[c, h, way],
            recv_sem=line_rsem.at[c, h, slot],
            device_id={"dp": target * 2 + inner},
            device_id_type=MESH,
        )

    def line_wait(c, h, slot):
        line_copy(c, h, slot, outer, 0).wait_recv()

    def own_sends(c, h, act):
        for way, hop in enumerate((2, -2, 1, -1)):
            @pl.when((outer + hop >= 0) & (outer + hop < lines))
            def _():
                act(line_copy(c, h, outer, outer + hop, way))

    def relays(c, h, step, side, act, arrive):
        slot = outer - side * 2 * step
        for n in range(2):
            hop = side * (n + 1)

            @pl.when((slot >= 0) & (slot < lines) & (outer + hop >= 0) & (outer + hop < lines))
            def _():
                if arrive and n == 0:
                    line_wait(c, h, slot)
                act(line_copy(c, h, slot, outer + hop, 4 * step + (side + 1) + n))

    def relay(c, h):
        for step in range(1, (lines + 1) // 2):
            for side in (1, -1):
                relays(c, h, step, side, lambda copy: copy.start(), True)

    def arrive(c, h):
        for slot in range(lines):
            gap = outer - slot
            far = gap if isinstance(gap, int) else jnp.abs(gap)
            onward = jnp.where(gap > 0, outer + 1 < lines, outer >= 1)
            passed = (lax.rem(far, 2) == 0) & onward

            @pl.when((far > 0) & jnp.logical_not(passed))
            def _():
                line_wait(c, h, slot)

    wanted = jnp.where(kind == 0, 1.0, 0.0)
    sums = [jnp.zeros((1, HEAD_DIM), F32), jnp.zeros((1, HEAD_DIM), F32)]

    def curve(c):
        first, rows = chunks[c]
        reach = first + rows
        span = slice(first, reach)
        chip_copy(c).wait_recv()
        whole = own_part[span, :] + chip_recv[span, :].astype(F32)
        shift = tokens[span, :].astype(F32) - targets[span, :].astype(F32)
        residual[kind, span, :] = ((whole + wanted * shift) * row_weights[span, :]).astype(BF16)
        res_copy(c, kind).start()
        back_own = dot(residual[kind, span, :], wo_turned[...])
        res_copy(c, other).wait_recv()
        back_other = dot(residual[other, span, :], wo_turned[...])
        back = jnp.where(kind == 0, back_own, back_other).astype(BF16)
        back_tangent = jnp.where(kind == 0, back_other, back_own).astype(BF16)
        cos_q = cos[span, :]
        sin_q = sin[span, :]
        for h in range(heads):
            cols = slice(h * HEAD_DIM, (h + 1) * HEAD_DIM)
            left = left_main[h, span, :]
            right = right_main[h, :reach, :]
            v = values[:reach, cols]
            p = soft[h, span, :reach]
            d_p = d_soft[h, span, :reach]
            u = dot(back[:, cols], v, NT)
            u_tangent = dot(back_tangent[:, cols], v, NT)
            centered = u - jnp.sum(p * u, axis=1, keepdims=True)
            level = jnp.sum(d_p * u + p * u_tangent, axis=1, keepdims=True)
            mixed = ((d_p * centered + p * (u_tangent - level)) * scale).astype(BF16)
            lead = (p * centered * scale).astype(BF16)
            hq = dot(mixed, right[:, :HEAD_DIM]) + dot(lead, right[:, HEAD_DIM:])
            hk = dot(mixed, left[:, HEAD_DIM:], TN) + dot(lead, left[:, :HEAD_DIM], TN)
            if c > 0:
                hk = hk_sum[:reach, cols] + hk
            if c < count - 1:
                hk_sum[:reach, cols] = hk
            hq = unrotate(hq, cos_q, sin_q)
            hk = unrotate(hk[span, :], cos_q, sin_q)
            hq = (hq.astype(BF16).astype(F32) * head_sign[0:1, cols]).astype(BF16)
            hk = (hk.astype(BF16).astype(F32) * head_sign[1:2, cols]).astype(BF16)
            gathered[h, outer, span, :HEAD_DIM] = hq
            gathered[h, outer, span, HEAD_DIM:] = hk
            own_sends(c, h, lambda copy: copy.start())
            probe = product[span, cols]
            sums[0] = sums[0] + jnp.sum(hq.astype(F32) * probe, axis=0, keepdims=True)
            sums[1] = sums[1] + jnp.sum(hk.astype(F32) * probe, axis=0, keepdims=True)

    attend(0)
    loads[4].wait()
    project(0)
    for c in range(1, count):
        attend(c)
        project(c)
    loads[5].wait()
    wo_turned[...] = jnp.transpose(wo[...])
    for step in range(1, lines):
        slab_copy(step).wait_recv()
        share_copy(step).start()
    slabs[outer] = signed[:, pl.ds(pl.multiple_of(outer * slab, slab), slab)]

    curve(0)
    for step in range(1, lines):
        share_copy(step).wait_recv()
    for o in range(lines):
        slabs_turned[:, o * seq : (o + 1) * seq] = jnp.transpose(slabs[o])
    for c in range(1, count):
        curve(c)
        for h in range(heads):
            relay(c - 1, h)

    lane = lax.broadcasted_iota(jnp.int32, (1, HEAD_DIM), 1)
    stat_send[0] = jnp.where(
        lane < HEAD_DIM // 2,
        jnp.sum(sums[0], axis=1, keepdims=True),
        jnp.sum(sums[1], axis=1, keepdims=True),
    )

    def stat_copy(n):
        target = ({"mp": pair}, {"mp": chip}, {"dp": x_peer})[n]
        return pltpu.make_async_remote_copy(
            src_ref=stat_send.at[n],
            dst_ref=stat_recv.at[n],
            send_sem=stat_ssem.at[n],
            recv_sem=stat_rsem.at[n],
            device_id=target,
            device_id_type=MESH,
        )

    def all_copy(step):
        return pltpu.make_async_remote_copy(
            src_ref=stat_all.at[outer],
            dst_ref=stat_all.at[outer],
            send_sem=all_ssem.at[step],
            recv_sem=all_rsem.at[step],
            device_id={"dp": lax.rem(outer + step, lines) * 2 + inner},
            device_id_type=MESH,
        )

    def x_copy(h):
        return pltpu.make_async_remote_copy(
            src_ref=x_send.at[h],
            dst_ref=x_recv.at[h],
            send_sem=x_ssem.at[h],
            recv_sem=x_rsem.at[h],
            device_id={"dp": x_peer},
            device_id_type=MESH,
        )

    stat_copy(0).start()
    own_rows = pl.ds(pl.multiple_of(inner * block, block), block)
    peer_rows = pl.ds(pl.multiple_of((1 - inner) * block, block), block)
    for h in range(heads):
        relay(count - 1, h)
        if h < 3:
            stat_copy(h).wait_recv()
            total = stat_send[h] + stat_recv[h]
            if h < 2:
                stat_send[h + 1] = total
                stat_copy(h + 1).start()
            else:
                stat_all[outer] = total
                for step in range(1, lines):
                    all_copy(step).start()
    for h in range(heads):
        for c in range(count):
            arrive(c, h)
        stack = gathered[h].reshape(lines * seq, PAIR)
        x_send[h] = dot(slabs_turned[peer_rows, :], stack).astype(BF16)
        x_copy(h).start()
        own_sum[h] = dot(slabs_turned[own_rows, :], stack)

    def out_copies(h):
        cols = pl.ds(h * HEAD_DIM, HEAD_DIM)
        return [
            pltpu.make_async_copy(result.at[n, :, cols], target.at[:, cols], out_sem.at[n, h])
            for n, target in enumerate((diag_query, diag_key))
        ]

    for h in range(heads):
        cols = slice(h * HEAD_DIM, (h + 1) * HEAD_DIM)
        signs = pattern[pl.ds(pl.multiple_of(dp * block, block), block), cols].astype(F32) * (1.0 / groups)
        x_copy(h).wait_recv()
        total = own_sum[h] + x_recv[h].astype(F32)
        result[0, :, cols] = total[:, :HEAD_DIM] * signs
        result[1, :, cols] = total[:, HEAD_DIM:] * signs
        for copy in out_copies(h):
            copy.start()
    for step in range(1, lines):
        all_copy(step).wait_recv()
    mean_out[...] = jnp.sum(stat_all[...], axis=0) * (1.0 / groups) / entries

    for step in range(1, lines):
        slab_copy(step).wait_send()
        share_copy(step).wait_send()
        all_copy(step).wait_send()
    for c in range(count):
        pair_copy(c).wait_send()
        chip_copy(c).wait_send()
        res_copy(c, kind).wait_send()
        for h in range(heads):
            own_sends(c, h, lambda copy: copy.wait_send())
            for step in range(1, (lines + 1) // 2):
                for side in (1, -1):
                    relays(c, h, step, side, lambda copy: copy.wait_send(), False)
    for n in range(3):
        stat_copy(n).wait_send()
    for h in range(heads):
        x_copy(h).wait_send()
        for copy in out_copies(h):
            copy.wait()


def local(
    tokens,
    targets,
    loss_weights,
    segments,
    probe_model,
    probe_heads,
    norm_gain,
    w_query,
    w_key,
    w_value,
    w_out,
):
    groups = lax.axis_size("dp")
    parts = lax.axis_size("mp")
    assert parts == 4 and groups % 2 == 0
    seq, width = tokens.shape
    feat = w_query.shape[1]
    heads = feat // HEAD_DIM
    block = width // groups
    lines = groups // 2
    quarter = seq // 4
    chunks = ((3 * quarter, quarter), (2 * quarter, quarter), (0, 2 * quarter))
    count = len(chunks)
    position = np.arange(seq, dtype=np.float32)
    exponent = np.arange(0, HEAD_DIM, 2).astype(np.float32) / np.float32(HEAD_DIM)
    angles = position[:, None] * (np.float32(10000.0) ** (-exponent)).astype(np.float32)[None, :]
    cos = np.cos(angles.astype(np.float64)).astype(np.float32)
    sin = np.sin(angles.astype(np.float64)).astype(np.float32)
    cosine = np.concatenate([cos, cos], axis=1)
    sine = np.concatenate([-sin, sin], axis=1)
    vmem = pl.BlockSpec(memory_space=pltpu.VMEM)
    anywhere = pl.BlockSpec(memory_space=pl.ANY)
    dma = pltpu.SemaphoreType.DMA
    ways = 4 + 4 * ((lines + 1) // 2 - 1) + 4
    diag_query, diag_key, means = pl.pallas_call(
        functools.partial(kernel, groups, parts, float(width * feat * parts), chunks),
        out_shape=(
            jax.ShapeDtypeStruct((block, feat), F32),
            jax.ShapeDtypeStruct((block, feat), F32),
            jax.ShapeDtypeStruct((1, HEAD_DIM), F32),
        ),
        in_specs=[vmem] * 7 + [anywhere] * 6,
        out_specs=(anywhere, anywhere, vmem),
        scratch_shapes=[
            pltpu.VMEM((seq, width), BF16),
            pltpu.VMEM((seq, width), BF16),
            pltpu.VMEM((width, feat), BF16),
            pltpu.VMEM((width, feat), BF16),
            pltpu.VMEM((width, feat), BF16),
            pltpu.VMEM((feat, width), BF16),
            pltpu.VMEM((width, feat), BF16),
            pltpu.VMEM((seq, width), BF16),
            pltpu.VMEM((seq, width), BF16),
            pltpu.VMEM((lines, seq, 2 * block), BF16),
            pltpu.VMEM((2 * block, lines * seq), BF16),
            pltpu.VMEM((width, feat), BF16),
            pltpu.VMEM((seq, feat), F32),
            pltpu.VMEM((heads, seq, PAIR), BF16),
            pltpu.VMEM((heads, seq, PAIR), BF16),
            pltpu.VMEM((heads, seq, PAIR), BF16),
            pltpu.VMEM((heads, seq, PAIR), BF16),
            pltpu.VMEM((seq, feat), BF16),
            pltpu.VMEM((heads, seq, seq), F32),
            pltpu.VMEM((heads, seq, seq), F32),
            pltpu.VMEM((2, seq, feat), BF16),
            pltpu.VMEM((seq, width), BF16),
            pltpu.VMEM((seq, width), F32),
            pltpu.VMEM((seq, width), BF16),
            pltpu.VMEM((seq, width), BF16),
            pltpu.VMEM((seq, width), BF16),
            pltpu.VMEM((2, seq, width), BF16),
            pltpu.VMEM((seq, feat), F32),
            pltpu.VMEM((heads, lines, seq, PAIR), BF16),
            pltpu.VMEM((heads, block, PAIR), BF16),
            pltpu.VMEM((heads, block, PAIR), BF16),
            pltpu.VMEM((heads, block, PAIR), F32),
            pltpu.VMEM((2, block, feat), F32),
            pltpu.VMEM((3, 1, HEAD_DIM), F32),
            pltpu.VMEM((3, 1, HEAD_DIM), F32),
            pltpu.VMEM((lines, 1, HEAD_DIM), F32),
            dma((6,)),
            dma((lines,)),
            dma((lines,)),
            dma((lines,)),
            dma((lines,)),
            dma((count,)),
            dma((count,)),
            dma((count,)),
            dma((count,)),
            dma((count,)),
            dma((count,)),
            dma((count, heads, ways)),
            dma((count, heads, lines)),
            dma((heads,)),
            dma((heads,)),
            dma((3,)),
            dma((3,)),
            dma((lines,)),
            dma((lines,)),
            dma((2, heads)),
        ],
        compiler_params=pltpu.CompilerParams(
            collective_id=0, has_side_effects=True, vmem_limit_bytes=58 * 1024 * 1024
        ),
    )(
        loss_weights.reshape(1, seq),
        segments,
        probe_model,
        probe_heads,
        norm_gain.reshape(1, width),
        jnp.asarray(cosine),
        jnp.asarray(sine),
        tokens,
        targets,
        w_query,
        w_key,
        w_value,
        w_out,
    )
    mean_diag = jnp.stack([means[0, 0], means[0, HEAD_DIM // 2]])
    return (diag_query, diag_key, mean_diag)


def solution(mesh):
    placed = (
        P("dp", None),
        P("dp", None),
        P("dp"),
        P("dp", None),
        P("dp", None),
        P("dp", None, "mp"),
        P(),
        P(None, "mp"),
        P(None, "mp"),
        P(None, "mp"),
        P("mp", None),
    )
    return jax.shard_map(
        local,
        mesh=mesh,
        in_specs=placed,
        out_specs=(P("dp", "mp"), P("dp", "mp"), P()),
        check_vma=False,
    )
```

```python
import functools

import jax
import jax.numpy as jnp
import numpy as np
from jax import lax
from jax.experimental import pallas as pl
from jax.experimental.pallas import tpu as pltpu
from jax.sharding import PartitionSpec as P

HEAD_DIM = 128
PAIR = 2 * HEAD_DIM
PRIME = 32749
SIZES = (2, 3, 5, 6)
F32 = jnp.float32
BF16 = jnp.bfloat16
MESH = pl.DeviceIdType.MESH

NN = (((1,), (0,)), ((), ()))
NT = (((1,), (1,)), ((), ()))
TN = (((0,), (0,)), ((), ()))


def dot(left, right, dims=NN):
    return lax.dot_general(left, right, dims, preferred_element_type=F32)


def low(left, right, dims=NN):
    return dot(left.astype(BF16), right.astype(BF16), dims)


def halves(array):
    high = array.astype(BF16)
    return high, (array - high.astype(F32)).astype(BF16)


def modulo(whole):
    times = (whole.astype(F32) * (1.0 / PRIME)).astype(jnp.int32)
    left = whole - times * PRIME
    left = jnp.where(left < 0, left + PRIME, left)
    return jnp.where(left >= PRIME, left - PRIME, left)


def wrap(value):
    return jnp.where(value >= PRIME, value - PRIME, value)


def fill_pattern(pattern, first_col, between):
    step = 16
    width, feat = pattern.shape
    rows = lax.broadcasted_iota(jnp.int32, (step, 1), 0) * 1103 + 7
    cols = modulo((first_col + lax.broadcasted_iota(jnp.int32, (1, feat), 1)) * 2713)
    start = wrap(rows + cols)
    jump = step * 1103 % PRIME
    square = modulo(start * start).astype(F32)
    change = modulo(start * (2 * jump) + jump * jump).astype(F32)
    bend = float(2 * jump * jump % PRIME)
    round_to = float(3 << 22)

    def body(n, state):
        square, change = state
        tenth = square * 0.1 + 0.05
        whole = (tenth + round_to) - round_to
        signs = jnp.where(tenth >= whole, 1.0, -1.0)
        pattern[pl.ds(pl.multiple_of(n * step, step), step), :] = signs.astype(BF16)
        return wrap(square + change), wrap(change + bend)

    middle = width // step // 2
    state = lax.fori_loop(0, middle, body, (square, change), unroll=4)
    between()
    lax.fori_loop(middle, width // step, body, state, unroll=4)


def rotate(array, cos, sin):
    return array * cos + pltpu.roll(array, HEAD_DIM // 2, 1) * sin


def unrotate(array, cos, sin):
    return array * cos - pltpu.roll(array, HEAD_DIM // 2, 1) * sin


def kernel(
    groups,
    parts,
    entries,
    chunks,
    weights_hbm,
    seg_hbm,
    model_hbm,
    head_hbm,
    gain_hbm,
    cosine_hbm,
    sine_hbm,
    tokens_hbm,
    targets_hbm,
    wq_hbm,
    wk_hbm,
    wv_hbm,
    wo_hbm,
    diag_query,
    diag_key,
    mean_out,
    weights_row,
    seg_row,
    model_bits,
    head_bits,
    gain,
    cosine,
    sine,
    tokens,
    targets,
    wq,
    wk,
    wv,
    wo,
    wo_turned,
    normed,
    signed,
    slabs,
    slabs_turned,
    pattern,
    product,
    left_main,
    left_rest,
    right_main,
    right_rest,
    values,
    soft,
    d_soft,
    attended,
    out_send,
    own_part,
    pair_recv,
    chip_send,
    chip_recv,
    residual,
    hk_sum,
    gathered,
    x_send,
    x_recv,
    own_sum,
    result,
    stat_send,
    stat_recv,
    stat_all,
    load_sem,
    slab_ssem,
    slab_rsem,
    share_ssem,
    share_rsem,
    pair_ssem,
    pair_rsem,
    chip_ssem,
    chip_rsem,
    res_ssem,
    res_rsem,
    line_ssem,
    line_rsem,
    x_ssem,
    x_rsem,
    stat_ssem,
    stat_rsem,
    all_ssem,
    all_rsem,
    out_sem,
    small_sem,
):
    seq, width = tokens.shape
    feat = wq.shape[1]
    heads = feat // HEAD_DIM
    block = width // groups
    lines = groups // 2
    slab = 2 * block
    half = seq // 2
    count = len(chunks)
    dp = lax.axis_index("dp")
    mp = lax.axis_index("mp")
    kind = lax.rem(mp, 2)
    other = 1 - kind
    pair = mp + 1 - 2 * kind
    chip = lax.rem(mp + 2, parts)
    inner = lax.rem(dp, 2)
    outer = dp // 2
    x_peer = dp + 1 - 2 * inner

    loads = []
    for n, (source, target) in enumerate(
        (
            (tokens_hbm, tokens),
            (wq_hbm, wq),
            (wk_hbm, wk),
            (wv_hbm, wv),
            (wo_hbm, wo),
            (targets_hbm, targets),
        )
    ):
        loads.append(pltpu.make_async_copy(source, target, load_sem.at[n]))
    loads[0].start()
    smalls = []
    for n, (source, target) in enumerate(
        (
            (model_hbm, model_bits),
            (gain_hbm, gain),
            (head_hbm, head_bits),
            (cosine_hbm, cosine),
            (sine_hbm, sine),
            (seg_hbm, seg_row),
            (weights_hbm, weights_row),
        )
    ):
        small = pltpu.make_async_copy(source, target, small_sem.at[n])
        small.start()
        smalls.append(small)

    barrier = pltpu.get_barrier_semaphore()
    for step in range(1, lines):
        peer = lax.rem(outer + step, lines) * 2 + inner
        pl.semaphore_signal(barrier, inc=1, device_id={"dp": peer}, device_id_type=MESH)
    pl.semaphore_signal(barrier, inc=1, device_id={"dp": x_peer}, device_id_type=MESH)
    pl.semaphore_signal(barrier, inc=1, device_id={"mp": pair}, device_id_type=MESH)
    pl.semaphore_signal(barrier, inc=1, device_id={"mp": chip}, device_id_type=MESH)

    def load_more():
        loads[1].start()
        loads[2].start()

    fill_pattern(pattern, mp * feat, load_more)

    for small in smalls:
        small.wait()
    model_sign = 2.0 * model_bits[...].astype(F32) - 1.0
    head_sign = 2.0 * head_bits[0].astype(F32) - 1.0
    loads[0].wait()
    token_float = tokens[...].astype(F32)
    inverse = lax.rsqrt(jnp.sum(token_float * token_float, axis=1, keepdims=True) / width + 1e-06)
    for start in range(0, width, 256):
        cols = slice(start, start + 256)
        part = (tokens[:, cols].astype(F32) * inverse * gain[:, cols]).astype(BF16)
        normed[:, cols] = part
        signed[:, cols] = (part.astype(F32) * model_sign[:, cols]).astype(BF16)

    for load in loads[3:]:
        load.start()
    pl.semaphore_wait(barrier, lines + 2)

    def slab_copy(step):
        peer = lax.rem(outer + step, lines)
        return pltpu.make_async_remote_copy(
            src_ref=signed.at[
                pl.ds(pl.multiple_of(kind * half, half), half),
                pl.ds(pl.multiple_of(peer * slab, slab), slab),
            ],
            dst_ref=slabs.at[outer, pl.ds(pl.multiple_of(kind * half, half), half), :],
            send_sem=slab_ssem.at[step],
            recv_sem=slab_rsem.at[step],
            device_id={"dp": peer * 2 + inner},
            device_id_type=MESH,
        )

    def share_copy(step):
        owner = lax.rem(outer - step + lines, lines)
        mine = slabs.at[owner, pl.ds(pl.multiple_of(kind * half, half), half), :]
        return pltpu.make_async_remote_copy(
            src_ref=mine,
            dst_ref=mine,
            send_sem=share_ssem.at[step],
            recv_sem=share_rsem.at[step],
            device_id={"mp": pair},
            device_id_type=MESH,
        )

    for step in range(1, lines):
        slab_copy(step).start()

    cos = cosine[...]
    sin = sine[...]
    scale = HEAD_DIM ** (-0.5)

    product[...] = dot(signed[...], pattern[...])
    for h in range(heads):
        cols = slice(h * HEAD_DIM, (h + 1) * HEAD_DIM)
        probe = product[:, cols]
        high, rest = halves(rotate(probe * head_sign[0:1, cols], cos, sin))
        left_main[h, :, :HEAD_DIM] = high
        left_rest[h, :, :HEAD_DIM] = rest
        high, rest = halves(rotate(probe * head_sign[1:2, cols], cos, sin))
        right_main[h, :, HEAD_DIM:] = high
        right_rest[h, :, HEAD_DIM:] = rest
    loads[1].wait()
    query = dot(normed[...], wq[...])
    for h in range(heads):
        cols = slice(h * HEAD_DIM, (h + 1) * HEAD_DIM)
        high, rest = halves(rotate(query[:, cols], cos, sin))
        left_main[h, :, HEAD_DIM:] = high
        left_rest[h, :, HEAD_DIM:] = rest
    loads[2].wait()
    keys = dot(normed[...], wk[...])
    for h in range(heads):
        cols = slice(h * HEAD_DIM, (h + 1) * HEAD_DIM)
        high, rest = halves(rotate(keys[:, cols], cos, sin))
        right_main[h, :, :HEAD_DIM] = high
        right_rest[h, :, :HEAD_DIM] = rest
    loads[3].wait()
    values[...] = dot(normed[...], wv[...]).astype(BF16)

    place_q = lax.broadcasted_iota(jnp.int32, (seq, seq), 0)
    place_k = lax.broadcasted_iota(jnp.int32, (seq, seq), 1)
    same = place_q == place_k
    segments = seg_row[...].astype(F32)
    seg_col = jnp.sum(jnp.where(same, segments, 0.0), axis=1, keepdims=True)
    row_weights = jnp.sum(jnp.where(same, weights_row[...], 0.0), axis=1, keepdims=True) / seq

    def pair_copy(c):
        first, rows = chunks[c]
        return pltpu.make_async_remote_copy(
            src_ref=out_send.at[pl.ds(first, rows), :],
            dst_ref=pair_recv.at[pl.ds(first, rows), :],
            send_sem=pair_ssem.at[c],
            recv_sem=pair_rsem.at[c],
            device_id={"mp": pair},
            device_id_type=MESH,
        )

    def chip_copy(c):
        first, rows = chunks[c]
        return pltpu.make_async_remote_copy(
            src_ref=chip_send.at[pl.ds(first, rows), :],
            dst_ref=chip_recv.at[pl.ds(first, rows), :],
            send_sem=chip_ssem.at[c],
            recv_sem=chip_rsem.at[c],
            device_id={"mp": chip},
            device_id_type=MESH,
        )

    def res_copy(c, which):
        first, rows = chunks[c]
        return pltpu.make_async_remote_copy(
            src_ref=residual.at[which, pl.ds(first, rows), :],
            dst_ref=residual.at[which, pl.ds(first, rows), :],
            send_sem=res_ssem.at[c],
            recv_sem=res_rsem.at[c],
            device_id={"mp": pair},
            device_id_type=MESH,
        )

    def attend(c):
        first, rows = chunks[c]
        reach = first + rows
        span = slice(first, reach)
        place = first + lax.broadcasted_iota(jnp.int32, (rows, reach), 0)
        place = jnp.concatenate([place] * heads, axis=0)
        owner = jnp.concatenate([seg_col[span, :]] * heads, axis=0)
        allowed = (place >= lax.broadcasted_iota(jnp.int32, (heads * rows, reach), 1)) & (
            owner == segments[:, :reach]
        )
        blank = jnp.zeros((rows, HEAD_DIM), BF16)
        scores, d_scores = [], []
        for h in range(heads):
            both = left_main[h, span, :]
            rest = left_rest[h, span, :]
            q = jnp.concatenate([both[:, HEAD_DIM:], blank], axis=1)
            q_rest = jnp.concatenate([rest[:, HEAD_DIM:], blank], axis=1)
            main = dot(jnp.concatenate([both, rest, q, q_rest], axis=0), right_main[h, :reach, :], NT)
            minor = dot(jnp.concatenate([both, q], axis=0), right_rest[h, :reach, :], NT)
            d_scores.append(main[:rows] + (main[rows : 2 * rows] + minor[:rows]))
            scores.append(main[2 * rows : 3 * rows] + (main[3 * rows :] + minor[rows:]))
        scores = jnp.concatenate(scores, axis=0) * scale
        d_scores = jnp.concatenate(d_scores, axis=0) * scale
        raised = jnp.where(allowed, jnp.exp(scores), 0.0)
        p = raised / jnp.sum(raised, axis=1, keepdims=True)
        d_p = p * (d_scores - jnp.sum(p * d_scores, axis=1, keepdims=True))
        soft[:, span, :reach] = p.reshape(heads, rows, reach)
        d_soft[:, span, :reach] = d_p.reshape(heads, rows, reach)
        p = p.astype(BF16)
        d_p = d_p.astype(BF16)
        for h in range(heads):
            cols = slice(h * HEAD_DIM, (h + 1) * HEAD_DIM)
            own = slice(h * rows, (h + 1) * rows)
            mixed = dot(jnp.concatenate([p[own], d_p[own]], axis=0), values[:reach, cols]).astype(BF16)
            attended[0, span, cols] = mixed[:rows]
            attended[1, span, cols] = mixed[rows:]

    def project(c):
        first, rows = chunks[c]
        span = slice(first, first + rows)
        out_send[span, :] = dot(attended[other, span, :], wo[...]).astype(BF16)
        pair_copy(c).start()
        own_part[span, :] = dot(attended[kind, span, :], wo[...])

    def forward(c):
        first, rows = chunks[c]
        span = slice(first, first + rows)
        pair_copy(c).wait_recv()
        summed = own_part[span, :] + pair_recv[span, :].astype(F32)
        own_part[span, :] = summed
        chip_send[span, :] = summed.astype(BF16)
        chip_copy(c).start()

    def line_copy(c, h, slot, target, way):
        first, rows = chunks[c]
        here = gathered.at[h, slot, pl.ds(first, rows), :]
        return pltpu.make_async_remote_copy(
            src_ref=here,
            dst_ref=here,
            send_sem=line_ssem.at[c, h, way],
            recv_sem=line_rsem.at[c, h, slot],
            device_id={"dp": target * 2 + inner},
            device_id_type=MESH,
        )

    def line_wait(c, h, slot):
        line_copy(c, h, slot, outer, 0).wait_recv()

    def own_sends(c, h, act):
        for way, hop in enumerate((2, -2, 1, -1)):
            @pl.when((outer + hop >= 0) & (outer + hop < lines))
            def _():
                act(line_copy(c, h, outer, outer + hop, way))

    def relays(c, h, step, side, act, arrive):
        slot = outer - side * 2 * step
        for n in range(2):
            hop = side * (n + 1)

            @pl.when((slot >= 0) & (slot < lines) & (outer + hop >= 0) & (outer + hop < lines))
            def _():
                if arrive and n == 0:
                    line_wait(c, h, slot)
                act(line_copy(c, h, slot, outer + hop, 4 * step + (side + 1) + n))

    def relay(c, h):
        for step in range(1, (lines + 1) // 2):
            for side in (1, -1):
                relays(c, h, step, side, lambda copy: copy.start(), True)

    def arrive(c, h):
        for slot in range(lines):
            gap = outer - slot
            far = jnp.abs(gap)
            onward = jnp.where(gap > 0, outer + 1 < lines, outer >= 1)
            passed = (lax.rem(far, 2) == 0) & onward

            @pl.when((far > 0) & jnp.logical_not(passed))
            def _():
                line_wait(c, h, slot)

    wanted = jnp.where(kind == 0, 1.0, 0.0)
    sums = [jnp.zeros((1, HEAD_DIM), F32), jnp.zeros((1, HEAD_DIM), F32)]

    def curve(c):
        first, rows = chunks[c]
        reach = first + rows
        span = slice(first, reach)
        chip_copy(c).wait_recv()
        whole = own_part[span, :] + chip_recv[span, :].astype(F32)
        shift = tokens[span, :].astype(F32) - targets[span, :].astype(F32)
        residual[kind, span, :] = ((whole + wanted * shift) * row_weights[span, :]).astype(BF16)
        res_copy(c, kind).start()
        back_own = dot(residual[kind, span, :], wo_turned[...])
        res_copy(c, other).wait_recv()
        back_other = dot(residual[other, span, :], wo_turned[...])
        back = jnp.where(kind == 0, back_own, back_other).astype(BF16)
        back_tangent = jnp.where(kind == 0, back_other, back_own).astype(BF16)
        cos_q = cos[span, :]
        sin_q = sin[span, :]
        u, u_tangent = [], []
        for h in range(heads):
            cols = slice(h * HEAD_DIM, (h + 1) * HEAD_DIM)
            pulled = dot(
                jnp.concatenate([back[:, cols], back_tangent[:, cols]], axis=0), values[:reach, cols], NT
            )
            u.append(pulled[:rows])
            u_tangent.append(pulled[rows:])
        u = jnp.concatenate(u, axis=0)
        u_tangent = jnp.concatenate(u_tangent, axis=0)
        p = soft[:, span, :reach].reshape(heads * rows, reach)
        d_p = d_soft[:, span, :reach].reshape(heads * rows, reach)
        centered = u - jnp.sum(p * u, axis=1, keepdims=True)
        level = jnp.sum(d_p * u + p * u_tangent, axis=1, keepdims=True)
        all_mixed = ((d_p * centered + p * (u_tangent - level)) * scale).astype(BF16)
        all_lead = (p * centered * scale).astype(BF16)
        for h in range(heads):
            cols = slice(h * HEAD_DIM, (h + 1) * HEAD_DIM)
            left = left_main[h, span, :]
            right = right_main[h, :reach, :]
            mixed = all_mixed[h * rows : (h + 1) * rows]
            lead = all_lead[h * rows : (h + 1) * rows]
            hq = dot(mixed, right[:, :HEAD_DIM]) + dot(lead, right[:, HEAD_DIM:])
            hk = dot(
                jnp.concatenate([mixed, lead], axis=0),
                jnp.concatenate([left[:, HEAD_DIM:], left[:, :HEAD_DIM]], axis=0),
                TN,
            )
            if c > 0:
                hk = hk_sum[:reach, cols] + hk
            if c < count - 1:
                hk_sum[:reach, cols] = hk
            hq = unrotate(hq, cos_q, sin_q)
            hk = unrotate(hk[span, :], cos_q, sin_q)
            hq = (hq.astype(BF16).astype(F32) * head_sign[0:1, cols]).astype(BF16)
            hk = (hk.astype(BF16).astype(F32) * head_sign[1:2, cols]).astype(BF16)
            gathered[h, outer, span, :HEAD_DIM] = hq
            gathered[h, outer, span, HEAD_DIM:] = hk
            own_sends(c, h, lambda copy: copy.start())
            probe = product[span, cols]
            sums[0] = sums[0] + jnp.sum(hq.astype(F32) * probe, axis=0, keepdims=True)
            sums[1] = sums[1] + jnp.sum(hk.astype(F32) * probe, axis=0, keepdims=True)

    def gather_slabs():
        for step in range(1, lines):
            slab_copy(step).wait_recv()
            share_copy(step).start()
        slabs[outer] = signed[:, pl.ds(pl.multiple_of(outer * slab, slab), slab)]

    def turn_slabs():
        for step in range(1, lines):
            share_copy(step).wait_recv()
        for o in range(lines):
            slabs_turned[:, o * seq : (o + 1) * seq] = jnp.transpose(slabs[o])

    attend(0)
    loads[4].wait()
    project(0)
    forward(0)
    for c in (1, 2):
        attend(c)
        project(c)
        forward(c)
    loads[5].wait()
    wo_turned[...] = jnp.transpose(wo[...])
    curve(0)
    for c in range(3, count):
        attend(c)
        project(c)
        forward(c)
    gather_slabs()
    curve(1)
    for h in range(heads):
        relay(0, h)
    turn_slabs()
    for c in range(2, count):
        curve(c)
        for h in range(heads):
            relay(c - 1, h)

    lane = lax.broadcasted_iota(jnp.int32, (1, HEAD_DIM), 1)
    stat_send[0] = jnp.where(
        lane < HEAD_DIM // 2,
        jnp.sum(sums[0], axis=1, keepdims=True),
        jnp.sum(sums[1], axis=1, keepdims=True),
    )

    def stat_copy(n):
        target = ({"mp": pair}, {"mp": chip}, {"dp": x_peer})[n]
        return pltpu.make_async_remote_copy(
            src_ref=stat_send.at[n],
            dst_ref=stat_recv.at[n],
            send_sem=stat_ssem.at[n],
            recv_sem=stat_rsem.at[n],
            device_id=target,
            device_id_type=MESH,
        )

    def all_copy(step):
        return pltpu.make_async_remote_copy(
            src_ref=stat_all.at[outer],
            dst_ref=stat_all.at[outer],
            send_sem=all_ssem.at[step],
            recv_sem=all_rsem.at[step],
            device_id={"dp": lax.rem(outer + step, lines) * 2 + inner},
            device_id_type=MESH,
        )

    def x_copy(h):
        return pltpu.make_async_remote_copy(
            src_ref=x_send.at[h],
            dst_ref=x_recv.at[h],
            send_sem=x_ssem.at[h],
            recv_sem=x_rsem.at[h],
            device_id={"dp": x_peer},
            device_id_type=MESH,
        )

    stat_copy(0).start()
    own_rows = pl.ds(pl.multiple_of(inner * block, block), block)
    peer_rows = pl.ds(pl.multiple_of((1 - inner) * block, block), block)
    for h in range(heads):
        relay(count - 1, h)
        for c in range(count):
            arrive(c, h)
        stack = gathered[h].reshape(lines * seq, PAIR)
        x_send[h] = dot(slabs_turned[peer_rows, :], stack).astype(BF16)
        x_copy(h).start()
        own_sum[h] = dot(slabs_turned[own_rows, :], stack)
        if h < 3:
            stat_copy(h).wait_recv()
            total = stat_send[h] + stat_recv[h]
            if h < 2:
                stat_send[h + 1] = total
                stat_copy(h + 1).start()
            else:
                stat_all[outer] = total
                for step in range(1, lines):
                    all_copy(step).start()

    def out_copies(h):
        cols = pl.ds(h * HEAD_DIM, HEAD_DIM)
        return [
            pltpu.make_async_copy(result.at[n, :, cols], target.at[:, cols], out_sem.at[n, h])
            for n, target in enumerate((diag_query, diag_key))
        ]

    for h in range(heads):
        cols = slice(h * HEAD_DIM, (h + 1) * HEAD_DIM)
        signs = pattern[pl.ds(pl.multiple_of(dp * block, block), block), cols].astype(F32) * (1.0 / groups)
        x_copy(h).wait_recv()
        total = own_sum[h] + x_recv[h].astype(F32)
        result[0, :, cols] = total[:, :HEAD_DIM] * signs
        result[1, :, cols] = total[:, HEAD_DIM:] * signs
        for copy in out_copies(h):
            copy.start()
    for step in range(1, lines):
        all_copy(step).wait_recv()
    mean_out[...] = jnp.sum(stat_all[...], axis=0) * (1.0 / groups) / entries

    for step in range(1, lines):
        slab_copy(step).wait_send()
        share_copy(step).wait_send()
        all_copy(step).wait_send()
    for c in range(count):
        pair_copy(c).wait_send()
        chip_copy(c).wait_send()
        res_copy(c, kind).wait_send()
        for h in range(heads):
            own_sends(c, h, lambda copy: copy.wait_send())
            for step in range(1, (lines + 1) // 2):
                for side in (1, -1):
                    relays(c, h, step, side, lambda copy: copy.wait_send(), False)
    for n in range(3):
        stat_copy(n).wait_send()
    for h in range(heads):
        x_copy(h).wait_send()
        for copy in out_copies(h):
            copy.wait()


def finish(query_in, key_in, mean_in, query_out, key_out, mean_out, held, sem):
    rows = query_in.shape[0] // 2
    moves = []
    for n, (source, target) in enumerate(((query_in, query_out), (key_in, key_out))):
        for part in range(2):
            span = pl.ds(part * rows, rows)
            slot = held.at[n, span, :]
            take = pltpu.make_async_copy(source.at[span, :], slot, sem.at[0, n, part])
            give = pltpu.make_async_copy(slot, target.at[span, :], sem.at[1, n, part])
            take.start()
            moves.append((take, give))
    mean_out[0] = mean_in[0, 0]
    mean_out[1] = mean_in[0, HEAD_DIM // 2]
    for take, give in moves:
        take.wait()
        give.start()
    for take, give in moves:
        give.wait()


def local(
    tokens,
    targets,
    loss_weights,
    segments,
    probe_model,
    probe_heads,
    norm_gain,
    w_query,
    w_key,
    w_value,
    w_out,
):
    groups = lax.axis_size("dp")
    parts = lax.axis_size("mp")
    assert parts == 4 and groups % 2 == 0
    seq, width = tokens.shape
    feat = w_query.shape[1]
    heads = feat // HEAD_DIM
    block = width // groups
    lines = groups // 2
    sizes = [part * seq // 16 for part in SIZES]
    chunks = tuple((seq - sum(sizes[: n + 1]), size) for n, size in enumerate(sizes))
    count = len(chunks)
    position = np.arange(seq, dtype=np.float32)
    exponent = np.arange(0, HEAD_DIM, 2).astype(np.float32) / np.float32(HEAD_DIM)
    angles = position[:, None] * (np.float32(10000.0) ** (-exponent)).astype(np.float32)[None, :]
    cos = np.cos(angles.astype(np.float64)).astype(np.float32)
    sin = np.sin(angles.astype(np.float64)).astype(np.float32)
    cosine = np.concatenate([cos, cos], axis=1)
    sine = np.concatenate([-sin, sin], axis=1)
    vmem = pl.BlockSpec(memory_space=pltpu.VMEM)
    anywhere = pl.BlockSpec(memory_space=pl.ANY)
    dma = pltpu.SemaphoreType.DMA
    ways = 4 + 4 * ((lines + 1) // 2 - 1) + 4
    diag_query, diag_key, means = pl.pallas_call(
        functools.partial(kernel, groups, parts, float(width * feat * parts), chunks),
        out_shape=(
            jax.ShapeDtypeStruct((block, feat), F32),
            jax.ShapeDtypeStruct((block, feat), F32),
            jax.ShapeDtypeStruct((1, HEAD_DIM), F32),
        ),
        in_specs=[pl.BlockSpec(memory_space=pltpu.HBM)] * 13,
        out_specs=(anywhere, anywhere, vmem),
        scratch_shapes=[
            pltpu.VMEM((1, seq), F32),
            pltpu.VMEM((1, seq), jnp.int32),
            pltpu.VMEM((1, width), jnp.int32),
            pltpu.VMEM((1, 2, feat), jnp.int32),
            pltpu.VMEM((1, width), F32),
            pltpu.VMEM((seq, HEAD_DIM), F32),
            pltpu.VMEM((seq, HEAD_DIM), F32),
            pltpu.VMEM((seq, width), BF16),
            pltpu.VMEM((seq, width), BF16),
            pltpu.VMEM((width, feat), BF16),
            pltpu.VMEM((width, feat), BF16),
            pltpu.VMEM((width, feat), BF16),
            pltpu.VMEM((feat, width), BF16),
            pltpu.VMEM((width, feat), BF16),
            pltpu.VMEM((seq, width), BF16),
            pltpu.VMEM((seq, width), BF16),
            pltpu.VMEM((lines, seq, 2 * block), BF16),
            pltpu.VMEM((2 * block, lines * seq), BF16),
            pltpu.VMEM((width, feat), BF16),
            pltpu.VMEM((seq, feat), F32),
            pltpu.VMEM((heads, seq, PAIR), BF16),
            pltpu.VMEM((heads, seq, PAIR), BF16),
            pltpu.VMEM((heads, seq, PAIR), BF16),
            pltpu.VMEM((heads, seq, PAIR), BF16),
            pltpu.VMEM((seq, feat), BF16),
            pltpu.VMEM((heads, seq, seq), F32),
            pltpu.VMEM((heads, seq, seq), F32),
            pltpu.VMEM((2, seq, feat), BF16),
            pltpu.VMEM((seq, width), BF16),
            pltpu.VMEM((seq, width), F32),
            pltpu.VMEM((seq, width), BF16),
            pltpu.VMEM((seq, width), BF16),
            pltpu.VMEM((seq, width), BF16),
            pltpu.VMEM((2, seq, width), BF16),
            pltpu.VMEM((seq, feat), F32),
            pltpu.VMEM((heads, lines, seq, PAIR), BF16),
            pltpu.VMEM((heads, block, PAIR), BF16),
            pltpu.VMEM((heads, block, PAIR), BF16),
            pltpu.VMEM((heads, block, PAIR), F32),
            pltpu.VMEM((2, block, feat), F32),
            pltpu.VMEM((3, 1, HEAD_DIM), F32),
            pltpu.VMEM((3, 1, HEAD_DIM), F32),
            pltpu.VMEM((lines, 1, HEAD_DIM), F32),
            dma((6,)),
            dma((lines,)),
            dma((lines,)),
            dma((lines,)),
            dma((lines,)),
            dma((count,)),
            dma((count,)),
            dma((count,)),
            dma((count,)),
            dma((count,)),
            dma((count,)),
            dma((count, heads, ways)),
            dma((count, heads, lines)),
            dma((heads,)),
            dma((heads,)),
            dma((3,)),
            dma((3,)),
            dma((lines,)),
            dma((lines,)),
            dma((2, heads)),
            dma((7,)),
        ],
        compiler_params=pltpu.CompilerParams(
            collective_id=0, has_side_effects=True, vmem_limit_bytes=62 * 1024 * 1024
        ),
    )(
        loss_weights.reshape(1, seq),
        segments,
        probe_model,
        probe_heads,
        norm_gain.reshape(1, width),
        jnp.asarray(cosine),
        jnp.asarray(sine),
        tokens,
        targets,
        w_query,
        w_key,
        w_value,
        w_out,
    )
    return pl.pallas_call(
        finish,
        out_shape=(
            jax.ShapeDtypeStruct((block, feat), F32),
            jax.ShapeDtypeStruct((block, feat), F32),
            jax.ShapeDtypeStruct((2,), F32),
        ),
        in_specs=[anywhere, anywhere, pl.BlockSpec(memory_space=pltpu.SMEM)],
        out_specs=(anywhere, anywhere, pl.BlockSpec(memory_space=pltpu.SMEM)),
        scratch_shapes=[pltpu.VMEM((2, block, feat), F32), dma((2, 2, 2))],
    )(diag_query, diag_key, means)


def solution(mesh):
    placed = (
        P("dp", None),
        P("dp", None),
        P("dp"),
        P("dp", None),
        P("dp", None),
        P("dp", None, "mp"),
        P(),
        P(None, "mp"),
        P(None, "mp"),
        P(None, "mp"),
        P("mp", None),
    )
    return jax.shard_map(
        local,
        mesh=mesh,
        in_specs=placed,
        out_specs=(P("dp", "mp"), P("dp", "mp"), P()),
        check_vma=False,
    )
```

```python
import functools

import jax
import jax.numpy as jnp
import numpy as np
from jax import lax
from jax.experimental import pallas as pl
from jax.experimental.pallas import tpu as pltpu
from jax.sharding import PartitionSpec as P

HEAD_DIM = 128
PAIR = 2 * HEAD_DIM
PRIME = 32749
SIZES = (2, 3, 5, 6)
F32 = jnp.float32
BF16 = jnp.bfloat16
MESH = pl.DeviceIdType.MESH

NN = (((1,), (0,)), ((), ()))
NT = (((1,), (1,)), ((), ()))
TN = (((0,), (0,)), ((), ()))


def dot(left, right, dims=NN):
    return lax.dot_general(left, right, dims, preferred_element_type=F32)


def low(left, right, dims=NN):
    return dot(left.astype(BF16), right.astype(BF16), dims)


def halves(array):
    high = array.astype(BF16)
    return high, (array - high.astype(F32)).astype(BF16)


def modulo(whole):
    times = (whole.astype(F32) * (1.0 / PRIME)).astype(jnp.int32)
    left = whole - times * PRIME
    left = jnp.where(left < 0, left + PRIME, left)
    return jnp.where(left >= PRIME, left - PRIME, left)


def wrap(value):
    return jnp.where(value >= PRIME, value - PRIME, value)


def fill_pattern(pattern, first_col, between):
    step = 16
    width, feat = pattern.shape
    rows = lax.broadcasted_iota(jnp.int32, (step, 1), 0) * 1103 + 7
    cols = modulo((first_col + lax.broadcasted_iota(jnp.int32, (1, feat), 1)) * 2713)
    start = wrap(rows + cols)
    jump = step * 1103 % PRIME
    square = modulo(start * start).astype(F32)
    change = modulo(start * (2 * jump) + jump * jump).astype(F32)
    bend = float(2 * jump * jump % PRIME)
    round_to = float(3 << 22)

    def body(n, state):
        square, change = state
        tenth = square * 0.1 + 0.05
        whole = (tenth + round_to) - round_to
        signs = jnp.where(tenth >= whole, 1.0, -1.0)
        pattern[pl.ds(pl.multiple_of(n * step, step), step), :] = signs.astype(BF16)
        return wrap(square + change), wrap(change + bend)

    middle = width // step // 2
    state = lax.fori_loop(0, middle, body, (square, change), unroll=4)
    between()
    lax.fori_loop(middle, width // step, body, state, unroll=4)


def rotate(array, cos, sin):
    return array * cos + pltpu.roll(array, HEAD_DIM // 2, 1) * sin


def unrotate(array, cos, sin):
    return array * cos - pltpu.roll(array, HEAD_DIM // 2, 1) * sin


def kernel(
    groups,
    parts,
    entries,
    chunks,
    weights_hbm,
    seg_hbm,
    model_hbm,
    head_hbm,
    gain_hbm,
    cosine_hbm,
    sine_hbm,
    tokens_hbm,
    targets_hbm,
    wq_hbm,
    wk_hbm,
    wv_hbm,
    wo_hbm,
    diag_query,
    diag_key,
    mean_out,
    weights_row,
    seg_row,
    model_bits,
    head_bits,
    gain,
    cosine,
    sine,
    tokens,
    targets,
    wq,
    wk,
    wv,
    wo,
    wo_turned,
    normed,
    signed,
    slabs,
    slabs_turned,
    pattern,
    product,
    left_main,
    left_rest,
    right_main,
    right_rest,
    values,
    soft,
    d_soft,
    attended,
    out_send,
    own_part,
    pair_recv,
    chip_send,
    chip_recv,
    residual,
    hk_sum,
    gathered,
    x_send,
    x_recv,
    own_sum,
    result,
    stat_send,
    stat_recv,
    stat_all,
    load_sem,
    slab_ssem,
    slab_rsem,
    share_ssem,
    share_rsem,
    pair_ssem,
    pair_rsem,
    chip_ssem,
    chip_rsem,
    res_ssem,
    res_rsem,
    line_ssem,
    line_rsem,
    x_ssem,
    x_rsem,
    stat_ssem,
    stat_rsem,
    all_ssem,
    all_rsem,
    out_sem,
    small_sem,
):
    seq, width = tokens.shape
    feat = wq.shape[1]
    heads = feat // HEAD_DIM
    block = width // groups
    lines = groups // 2
    slab = 2 * block
    half = seq // 2
    count = len(chunks)
    dp = lax.axis_index("dp")
    mp = lax.axis_index("mp")
    kind = lax.rem(mp, 2)
    other = 1 - kind
    pair = mp + 1 - 2 * kind
    chip = lax.rem(mp + 2, parts)
    inner = lax.rem(dp, 2)
    outer = dp // 2
    x_peer = dp + 1 - 2 * inner

    loads = []
    for n, (source, target) in enumerate(
        (
            (tokens_hbm, tokens),
            (wq_hbm, wq),
            (wk_hbm, wk),
            (wv_hbm, wv),
            (wo_hbm, wo),
            (targets_hbm, targets),
        )
    ):
        loads.append(pltpu.make_async_copy(source, target, load_sem.at[n]))
    loads[0].start()
    smalls = []
    for n, (source, target) in enumerate(
        (
            (model_hbm, model_bits),
            (gain_hbm, gain),
            (head_hbm, head_bits),
            (cosine_hbm, cosine),
            (sine_hbm, sine),
            (seg_hbm, seg_row),
            (weights_hbm, weights_row),
        )
    ):
        small = pltpu.make_async_copy(source, target, small_sem.at[n])
        small.start()
        smalls.append(small)

    barrier = pltpu.get_barrier_semaphore()
    for step in range(1, lines):
        peer = lax.rem(outer + step, lines) * 2 + inner
        pl.semaphore_signal(barrier, inc=1, device_id={"dp": peer}, device_id_type=MESH)
    pl.semaphore_signal(barrier, inc=1, device_id={"dp": x_peer}, device_id_type=MESH)
    pl.semaphore_signal(barrier, inc=1, device_id={"mp": pair}, device_id_type=MESH)
    pl.semaphore_signal(barrier, inc=1, device_id={"mp": chip}, device_id_type=MESH)

    def load_more():
        loads[1].start()
        loads[2].start()

    fill_pattern(pattern, mp * feat, load_more)

    for small in smalls:
        small.wait()
    model_sign = 2.0 * model_bits[...].astype(F32) - 1.0
    head_sign = 2.0 * head_bits[0].astype(F32) - 1.0
    loads[0].wait()
    token_float = tokens[...].astype(F32)
    inverse = lax.rsqrt(jnp.sum(token_float * token_float, axis=1, keepdims=True) / width + 1e-06)
    for start in range(0, width, 256):
        cols = slice(start, start + 256)
        part = (tokens[:, cols].astype(F32) * inverse * gain[:, cols]).astype(BF16)
        normed[:, cols] = part
        signed[:, cols] = (part.astype(F32) * model_sign[:, cols]).astype(BF16)

    for load in loads[3:]:
        load.start()
    pl.semaphore_wait(barrier, lines + 2)

    def slab_copy(step):
        peer = lax.rem(outer + step, lines)
        return pltpu.make_async_remote_copy(
            src_ref=signed.at[
                pl.ds(pl.multiple_of(kind * half, half), half),
                pl.ds(pl.multiple_of(peer * slab, slab), slab),
            ],
            dst_ref=slabs.at[outer, pl.ds(pl.multiple_of(kind * half, half), half), :],
            send_sem=slab_ssem.at[step],
            recv_sem=slab_rsem.at[step],
            device_id={"dp": peer * 2 + inner},
            device_id_type=MESH,
        )

    def share_copy(step):
        owner = lax.rem(outer - step + lines, lines)
        mine = slabs.at[owner, pl.ds(pl.multiple_of(kind * half, half), half), :]
        return pltpu.make_async_remote_copy(
            src_ref=mine,
            dst_ref=mine,
            send_sem=share_ssem.at[step],
            recv_sem=share_rsem.at[step],
            device_id={"mp": pair},
            device_id_type=MESH,
        )

    for step in range(1, lines):
        slab_copy(step).start()

    cos = cosine[...]
    sin = sine[...]
    scale = HEAD_DIM ** (-0.5)

    product[...] = dot(signed[...], pattern[...])
    for h in range(heads):
        cols = slice(h * HEAD_DIM, (h + 1) * HEAD_DIM)
        probe = product[:, cols]
        high, rest = halves(rotate(probe * head_sign[0:1, cols], cos, sin))
        left_main[h, :, :HEAD_DIM] = high
        left_rest[h, :, :HEAD_DIM] = rest
        high, rest = halves(rotate(probe * head_sign[1:2, cols], cos, sin))
        right_main[h, :, HEAD_DIM:] = high
        right_rest[h, :, HEAD_DIM:] = rest
    loads[1].wait()
    query = dot(normed[...], wq[...])
    for h in range(heads):
        cols = slice(h * HEAD_DIM, (h + 1) * HEAD_DIM)
        high, rest = halves(rotate(query[:, cols], cos, sin))
        left_main[h, :, HEAD_DIM:] = high
        left_rest[h, :, HEAD_DIM:] = rest
    loads[2].wait()
    keys = dot(normed[...], wk[...])
    for h in range(heads):
        cols = slice(h * HEAD_DIM, (h + 1) * HEAD_DIM)
        high, rest = halves(rotate(keys[:, cols], cos, sin))
        right_main[h, :, :HEAD_DIM] = high
        right_rest[h, :, :HEAD_DIM] = rest
    loads[3].wait()
    values[...] = dot(normed[...], wv[...]).astype(BF16)

    place_q = lax.broadcasted_iota(jnp.int32, (seq, seq), 0)
    place_k = lax.broadcasted_iota(jnp.int32, (seq, seq), 1)
    same = place_q == place_k
    segments = seg_row[...].astype(F32)
    seg_col = jnp.sum(jnp.where(same, segments, 0.0), axis=1, keepdims=True)
    row_weights = jnp.sum(jnp.where(same, weights_row[...], 0.0), axis=1, keepdims=True) / seq

    def pair_copy(c):
        first, rows = chunks[c]
        return pltpu.make_async_remote_copy(
            src_ref=out_send.at[pl.ds(first, rows), :],
            dst_ref=pair_recv.at[pl.ds(first, rows), :],
            send_sem=pair_ssem.at[c],
            recv_sem=pair_rsem.at[c],
            device_id={"mp": pair},
            device_id_type=MESH,
        )

    def chip_copy(c):
        first, rows = chunks[c]
        return pltpu.make_async_remote_copy(
            src_ref=chip_send.at[pl.ds(first, rows), :],
            dst_ref=chip_recv.at[pl.ds(first, rows), :],
            send_sem=chip_ssem.at[c],
            recv_sem=chip_rsem.at[c],
            device_id={"mp": chip},
            device_id_type=MESH,
        )

    def res_copy(c, which):
        first, rows = chunks[c]
        return pltpu.make_async_remote_copy(
            src_ref=residual.at[which, pl.ds(first, rows), :],
            dst_ref=residual.at[which, pl.ds(first, rows), :],
            send_sem=res_ssem.at[c],
            recv_sem=res_rsem.at[c],
            device_id={"mp": pair},
            device_id_type=MESH,
        )

    def attend(c):
        first, rows = chunks[c]
        reach = first + rows
        span = slice(first, reach)
        place = first + lax.broadcasted_iota(jnp.int32, (rows, reach), 0)
        place = jnp.concatenate([place] * heads, axis=0)
        owner = jnp.concatenate([seg_col[span, :]] * heads, axis=0)
        allowed = (place >= lax.broadcasted_iota(jnp.int32, (heads * rows, reach), 1)) & (
            owner == segments[:, :reach]
        )
        blank = jnp.zeros((rows, HEAD_DIM), BF16)
        scores, d_scores = [], []
        for h in range(heads):
            both = left_main[h, span, :]
            rest = left_rest[h, span, :]
            q = jnp.concatenate([both[:, HEAD_DIM:], blank], axis=1)
            q_rest = jnp.concatenate([rest[:, HEAD_DIM:], blank], axis=1)
            main = dot(jnp.concatenate([both, rest, q, q_rest], axis=0), right_main[h, :reach, :], NT)
            minor = dot(jnp.concatenate([both, q], axis=0), right_rest[h, :reach, :], NT)
            d_scores.append(main[:rows] + (main[rows : 2 * rows] + minor[:rows]))
            scores.append(main[2 * rows : 3 * rows] + (main[3 * rows :] + minor[rows:]))
        scores = jnp.concatenate(scores, axis=0) * scale
        d_scores = jnp.concatenate(d_scores, axis=0) * scale
        raised = jnp.where(allowed, jnp.exp(scores), 0.0)
        p = raised / jnp.sum(raised, axis=1, keepdims=True)
        d_p = p * (d_scores - jnp.sum(p * d_scores, axis=1, keepdims=True))
        soft[:, span, :reach] = p.reshape(heads, rows, reach)
        d_soft[:, span, :reach] = d_p.reshape(heads, rows, reach)
        p = p.astype(BF16)
        d_p = d_p.astype(BF16)
        for h in range(heads):
            cols = slice(h * HEAD_DIM, (h + 1) * HEAD_DIM)
            own = slice(h * rows, (h + 1) * rows)
            mixed = dot(jnp.concatenate([p[own], d_p[own]], axis=0), values[:reach, cols]).astype(BF16)
            attended[0, span, cols] = mixed[:rows]
            attended[1, span, cols] = mixed[rows:]

    def project(c):
        first, rows = chunks[c]
        span = slice(first, first + rows)
        out_send[span, :] = dot(attended[other, span, :], wo[...]).astype(BF16)
        pair_copy(c).start()
        own_part[span, :] = dot(attended[kind, span, :], wo[...])

    def forward(c):
        first, rows = chunks[c]
        span = slice(first, first + rows)
        pair_copy(c).wait_recv()
        summed = own_part[span, :] + pair_recv[span, :].astype(F32)
        own_part[span, :] = summed
        chip_send[span, :] = summed.astype(BF16)
        chip_copy(c).start()

    def line_copy(c, h, slot, target, way):
        first, rows = chunks[c]
        here = gathered.at[h, slot, pl.ds(first, rows), :]
        return pltpu.make_async_remote_copy(
            src_ref=here,
            dst_ref=here,
            send_sem=line_ssem.at[c, h, way],
            recv_sem=line_rsem.at[c, h, slot],
            device_id={"dp": target * 2 + inner},
            device_id_type=MESH,
        )

    def line_wait(c, h, slot):
        line_copy(c, h, slot, outer, 0).wait_recv()

    def own_sends(c, h, act, near=True, far=True):
        for way, hop in enumerate((2, -2, 1, -1)):
            if not (near if abs(hop) == 1 else far):
                continue

            @pl.when((outer + hop >= 0) & (outer + hop < lines))
            def _():
                act(line_copy(c, h, outer, outer + hop, way))

    def relays(c, h, step, side, act, arrive):
        slot = outer - side * 2 * step
        for n in range(2):
            hop = side * (n + 1)

            @pl.when((slot >= 0) & (slot < lines) & (outer + hop >= 0) & (outer + hop < lines))
            def _():
                if arrive and n == 0:
                    line_wait(c, h, slot)
                act(line_copy(c, h, slot, outer + hop, 4 * step + (side + 1) + n))

    def relay(c, h):
        for step in range(1, (lines + 1) // 2):
            for side in (1, -1):
                relays(c, h, step, side, lambda copy: copy.start(), True)

    def arrive(c, h):
        for slot in range(lines):
            gap = outer - slot
            far = jnp.abs(gap)
            onward = jnp.where(gap > 0, outer + 1 < lines, outer >= 1)
            passed = (lax.rem(far, 2) == 0) & onward

            @pl.when((far > 0) & jnp.logical_not(passed))
            def _():
                line_wait(c, h, slot)

    wanted = jnp.where(kind == 0, 1.0, 0.0)
    sums = [jnp.zeros((1, HEAD_DIM), F32), jnp.zeros((1, HEAD_DIM), F32)]

    def curve(c):
        first, rows = chunks[c]
        reach = first + rows
        span = slice(first, reach)
        chip_copy(c).wait_recv()
        whole = own_part[span, :] + chip_recv[span, :].astype(F32)
        shift = tokens[span, :].astype(F32) - targets[span, :].astype(F32)
        residual[kind, span, :] = ((whole + wanted * shift) * row_weights[span, :]).astype(BF16)
        res_copy(c, kind).start()
        back_own = dot(residual[kind, span, :], wo_turned[...])
        res_copy(c, other).wait_recv()
        back_other = dot(residual[other, span, :], wo_turned[...])
        back = jnp.where(kind == 0, back_own, back_other).astype(BF16)
        back_tangent = jnp.where(kind == 0, back_other, back_own).astype(BF16)
        cos_q = cos[span, :]
        sin_q = sin[span, :]
        u, u_tangent = [], []
        for h in range(heads):
            cols = slice(h * HEAD_DIM, (h + 1) * HEAD_DIM)
            pulled = dot(
                jnp.concatenate([back[:, cols], back_tangent[:, cols]], axis=0), values[:reach, cols], NT
            )
            u.append(pulled[:rows])
            u_tangent.append(pulled[rows:])
        u = jnp.concatenate(u, axis=0)
        u_tangent = jnp.concatenate(u_tangent, axis=0)
        p = soft[:, span, :reach].reshape(heads * rows, reach)
        d_p = d_soft[:, span, :reach].reshape(heads * rows, reach)
        centered = u - jnp.sum(p * u, axis=1, keepdims=True)
        level = jnp.sum(d_p * u + p * u_tangent, axis=1, keepdims=True)
        all_mixed = ((d_p * centered + p * (u_tangent - level)) * scale).astype(BF16)
        all_lead = (p * centered * scale).astype(BF16)
        for h in range(heads):
            cols = slice(h * HEAD_DIM, (h + 1) * HEAD_DIM)
            left = left_main[h, span, :]
            right = right_main[h, :reach, :]
            mixed = all_mixed[h * rows : (h + 1) * rows]
            lead = all_lead[h * rows : (h + 1) * rows]
            hq = dot(mixed, right[:, :HEAD_DIM]) + dot(lead, right[:, HEAD_DIM:])
            hk = dot(
                jnp.concatenate([mixed, lead], axis=0),
                jnp.concatenate([left[:, HEAD_DIM:], left[:, :HEAD_DIM]], axis=0),
                TN,
            )
            if c > 0:
                hk = hk_sum[:reach, cols] + hk
            if c < count - 1:
                hk_sum[:reach, cols] = hk
            hq = unrotate(hq, cos_q, sin_q)
            hk = unrotate(hk[span, :], cos_q, sin_q)
            hq = (hq.astype(BF16).astype(F32) * head_sign[0:1, cols]).astype(BF16)
            hk = (hk.astype(BF16).astype(F32) * head_sign[1:2, cols]).astype(BF16)
            gathered[h, outer, span, :HEAD_DIM] = hq
            gathered[h, outer, span, HEAD_DIM:] = hk
            own_sends(c, h, lambda copy: copy.start(), near=c < count - 1)
            probe = product[span, cols]
            sums[0] = sums[0] + jnp.sum(hq.astype(F32) * probe, axis=0, keepdims=True)
            sums[1] = sums[1] + jnp.sum(hk.astype(F32) * probe, axis=0, keepdims=True)

    def gather_slabs():
        for step in range(1, lines):
            slab_copy(step).wait_recv()
            share_copy(step).start()
        slabs[outer] = signed[:, pl.ds(pl.multiple_of(outer * slab, slab), slab)]

    def turn_slabs():
        for step in range(1, lines):
            share_copy(step).wait_recv()
        for o in range(lines):
            slabs_turned[:, o * seq : (o + 1) * seq] = jnp.transpose(slabs[o])

    attend(0)
    loads[4].wait()
    project(0)
    forward(0)
    for c in (1, 2):
        attend(c)
        project(c)
        forward(c)
    loads[5].wait()
    wo_turned[...] = jnp.transpose(wo[...])
    curve(0)
    for c in range(3, count):
        attend(c)
        project(c)
        forward(c)
    gather_slabs()
    curve(1)
    for h in range(heads):
        relay(0, h)
    turn_slabs()
    for c in range(2, count):
        curve(c)
        for h in range(heads):
            relay(c - 1, h)

    lane = lax.broadcasted_iota(jnp.int32, (1, HEAD_DIM), 1)
    stat_send[0] = jnp.where(
        lane < HEAD_DIM // 2,
        jnp.sum(sums[0], axis=1, keepdims=True),
        jnp.sum(sums[1], axis=1, keepdims=True),
    )

    def stat_copy(n):
        target = ({"mp": pair}, {"mp": chip}, {"dp": x_peer})[n]
        return pltpu.make_async_remote_copy(
            src_ref=stat_send.at[n],
            dst_ref=stat_recv.at[n],
            send_sem=stat_ssem.at[n],
            recv_sem=stat_rsem.at[n],
            device_id=target,
            device_id_type=MESH,
        )

    def all_copy(step):
        return pltpu.make_async_remote_copy(
            src_ref=stat_all.at[outer],
            dst_ref=stat_all.at[outer],
            send_sem=all_ssem.at[step],
            recv_sem=all_rsem.at[step],
            device_id={"dp": lax.rem(outer + step, lines) * 2 + inner},
            device_id_type=MESH,
        )

    def x_copy(h):
        return pltpu.make_async_remote_copy(
            src_ref=x_send.at[h],
            dst_ref=x_recv.at[h],
            send_sem=x_ssem.at[h],
            recv_sem=x_rsem.at[h],
            device_id={"dp": x_peer},
            device_id_type=MESH,
        )

    stat_copy(0).start()
    own_rows = pl.ds(pl.multiple_of(inner * block, block), block)
    peer_rows = pl.ds(pl.multiple_of((1 - inner) * block, block), block)
    for h in range(heads):
        own_sends(count - 1, h, lambda copy: copy.start(), far=False)
        relay(count - 1, h)
    for h in range(heads):
        for c in range(count):
            arrive(c, h)
        stack = gathered[h].reshape(lines * seq, PAIR)
        x_send[h] = dot(slabs_turned[peer_rows, :], stack).astype(BF16)
        x_copy(h).start()
        own_sum[h] = dot(slabs_turned[own_rows, :], stack)
        if h < 3:
            stat_copy(h).wait_recv()
            total = stat_send[h] + stat_recv[h]
            if h < 2:
                stat_send[h + 1] = total
                stat_copy(h + 1).start()
            else:
                stat_all[outer] = total
                for step in range(1, lines):
                    all_copy(step).start()

    def out_copies(h):
        cols = pl.ds(h * HEAD_DIM, HEAD_DIM)
        return [
            pltpu.make_async_copy(result.at[n, :, cols], target.at[:, cols], out_sem.at[n, h])
            for n, target in enumerate((diag_query, diag_key))
        ]

    for h in range(heads):
        cols = slice(h * HEAD_DIM, (h + 1) * HEAD_DIM)
        signs = pattern[pl.ds(pl.multiple_of(dp * block, block), block), cols].astype(F32) * (1.0 / groups)
        x_copy(h).wait_recv()
        total = own_sum[h] + x_recv[h].astype(F32)
        result[0, :, cols] = total[:, :HEAD_DIM] * signs
        result[1, :, cols] = total[:, HEAD_DIM:] * signs
        for copy in out_copies(h):
            copy.start()
    for step in range(1, lines):
        all_copy(step).wait_recv()
    mean_out[...] = jnp.sum(stat_all[...], axis=0) * (1.0 / groups) / entries

    for step in range(1, lines):
        slab_copy(step).wait_send()
        share_copy(step).wait_send()
        all_copy(step).wait_send()
    for c in range(count):
        pair_copy(c).wait_send()
        chip_copy(c).wait_send()
        res_copy(c, kind).wait_send()
        for h in range(heads):
            own_sends(c, h, lambda copy: copy.wait_send())
            for step in range(1, (lines + 1) // 2):
                for side in (1, -1):
                    relays(c, h, step, side, lambda copy: copy.wait_send(), False)
    for n in range(3):
        stat_copy(n).wait_send()
    for h in range(heads):
        x_copy(h).wait_send()
        for copy in out_copies(h):
            copy.wait()


def finish(query_in, key_in, mean_in, query_out, key_out, mean_out, held, sem):
    rows = query_in.shape[0] // 2
    moves = []
    for n, (source, target) in enumerate(((query_in, query_out), (key_in, key_out))):
        for part in range(2):
            span = pl.ds(part * rows, rows)
            slot = held.at[n, span, :]
            take = pltpu.make_async_copy(source.at[span, :], slot, sem.at[0, n, part])
            give = pltpu.make_async_copy(slot, target.at[span, :], sem.at[1, n, part])
            take.start()
            moves.append((take, give))
    mean_out[0] = mean_in[0, 0]
    mean_out[1] = mean_in[0, HEAD_DIM // 2]
    for take, give in moves:
        take.wait()
        give.start()
    for take, give in moves:
        give.wait()


def local(
    tokens,
    targets,
    loss_weights,
    segments,
    probe_model,
    probe_heads,
    norm_gain,
    w_query,
    w_key,
    w_value,
    w_out,
):
    groups = lax.axis_size("dp")
    parts = lax.axis_size("mp")
    assert parts == 4 and groups % 2 == 0
    seq, width = tokens.shape
    feat = w_query.shape[1]
    heads = feat // HEAD_DIM
    block = width // groups
    lines = groups // 2
    sizes = [part * seq // 16 for part in SIZES]
    chunks = tuple((seq - sum(sizes[: n + 1]), size) for n, size in enumerate(sizes))
    count = len(chunks)
    position = np.arange(seq, dtype=np.float32)
    exponent = np.arange(0, HEAD_DIM, 2).astype(np.float32) / np.float32(HEAD_DIM)
    angles = position[:, None] * (np.float32(10000.0) ** (-exponent)).astype(np.float32)[None, :]
    cos = np.cos(angles.astype(np.float64)).astype(np.float32)
    sin = np.sin(angles.astype(np.float64)).astype(np.float32)
    cosine = np.concatenate([cos, cos], axis=1)
    sine = np.concatenate([-sin, sin], axis=1)
    vmem = pl.BlockSpec(memory_space=pltpu.VMEM)
    anywhere = pl.BlockSpec(memory_space=pl.ANY)
    dma = pltpu.SemaphoreType.DMA
    ways = 4 + 4 * ((lines + 1) // 2 - 1) + 4
    diag_query, diag_key, means = pl.pallas_call(
        functools.partial(kernel, groups, parts, float(width * feat * parts), chunks),
        out_shape=(
            jax.ShapeDtypeStruct((block, feat), F32),
            jax.ShapeDtypeStruct((block, feat), F32),
            jax.ShapeDtypeStruct((1, HEAD_DIM), F32),
        ),
        in_specs=[pl.BlockSpec(memory_space=pltpu.HBM)] * 13,
        out_specs=(anywhere, anywhere, vmem),
        scratch_shapes=[
            pltpu.VMEM((1, seq), F32),
            pltpu.VMEM((1, seq), jnp.int32),
            pltpu.VMEM((1, width), jnp.int32),
            pltpu.VMEM((1, 2, feat), jnp.int32),
            pltpu.VMEM((1, width), F32),
            pltpu.VMEM((seq, HEAD_DIM), F32),
            pltpu.VMEM((seq, HEAD_DIM), F32),
            pltpu.VMEM((seq, width), BF16),
            pltpu.VMEM((seq, width), BF16),
            pltpu.VMEM((width, feat), BF16),
            pltpu.VMEM((width, feat), BF16),
            pltpu.VMEM((width, feat), BF16),
            pltpu.VMEM((feat, width), BF16),
            pltpu.VMEM((width, feat), BF16),
            pltpu.VMEM((seq, width), BF16),
            pltpu.VMEM((seq, width), BF16),
            pltpu.VMEM((lines, seq, 2 * block), BF16),
            pltpu.VMEM((2 * block, lines * seq), BF16),
            pltpu.VMEM((width, feat), BF16),
            pltpu.VMEM((seq, feat), F32),
            pltpu.VMEM((heads, seq, PAIR), BF16),
            pltpu.VMEM((heads, seq, PAIR), BF16),
            pltpu.VMEM((heads, seq, PAIR), BF16),
            pltpu.VMEM((heads, seq, PAIR), BF16),
            pltpu.VMEM((seq, feat), BF16),
            pltpu.VMEM((heads, seq, seq), F32),
            pltpu.VMEM((heads, seq, seq), F32),
            pltpu.VMEM((2, seq, feat), BF16),
            pltpu.VMEM((seq, width), BF16),
            pltpu.VMEM((seq, width), F32),
            pltpu.VMEM((seq, width), BF16),
            pltpu.VMEM((seq, width), BF16),
            pltpu.VMEM((seq, width), BF16),
            pltpu.VMEM((2, seq, width), BF16),
            pltpu.VMEM((seq, feat), F32),
            pltpu.VMEM((heads, lines, seq, PAIR), BF16),
            pltpu.VMEM((heads, block, PAIR), BF16),
            pltpu.VMEM((heads, block, PAIR), BF16),
            pltpu.VMEM((heads, block, PAIR), F32),
            pltpu.VMEM((2, block, feat), F32),
            pltpu.VMEM((3, 1, HEAD_DIM), F32),
            pltpu.VMEM((3, 1, HEAD_DIM), F32),
            pltpu.VMEM((lines, 1, HEAD_DIM), F32),
            dma((6,)),
            dma((lines,)),
            dma((lines,)),
            dma((lines,)),
            dma((lines,)),
            dma((count,)),
            dma((count,)),
            dma((count,)),
            dma((count,)),
            dma((count,)),
            dma((count,)),
            dma((count, heads, ways)),
            dma((count, heads, lines)),
            dma((heads,)),
            dma((heads,)),
            dma((3,)),
            dma((3,)),
            dma((lines,)),
            dma((lines,)),
            dma((2, heads)),
            dma((7,)),
        ],
        compiler_params=pltpu.CompilerParams(
            collective_id=0, has_side_effects=True, vmem_limit_bytes=62 * 1024 * 1024
        ),
    )(
        loss_weights.reshape(1, seq),
        segments,
        probe_model,
        probe_heads,
        norm_gain.reshape(1, width),
        jnp.asarray(cosine),
        jnp.asarray(sine),
        tokens,
        targets,
        w_query,
        w_key,
        w_value,
        w_out,
    )
    return pl.pallas_call(
        finish,
        out_shape=(
            jax.ShapeDtypeStruct((block, feat), F32),
            jax.ShapeDtypeStruct((block, feat), F32),
            jax.ShapeDtypeStruct((2,), F32),
        ),
        in_specs=[anywhere, anywhere, pl.BlockSpec(memory_space=pltpu.SMEM)],
        out_specs=(anywhere, anywhere, pl.BlockSpec(memory_space=pltpu.SMEM)),
        scratch_shapes=[pltpu.VMEM((2, block, feat), F32), dma((2, 2, 2))],
    )(diag_query, diag_key, means)


def solution(mesh):
    placed = (
        P("dp", None),
        P("dp", None),
        P("dp"),
        P("dp", None),
        P("dp", None),
        P("dp", None, "mp"),
        P(),
        P(None, "mp"),
        P(None, "mp"),
        P(None, "mp"),
        P("mp", None),
    )
    return jax.shard_map(
        local,
        mesh=mesh,
        in_specs=placed,
        out_specs=(P("dp", "mp"), P("dp", "mp"), P()),
        check_vma=False,
    )
```

```python
import functools

import jax
import jax.numpy as jnp
import numpy as np
from jax import lax
from jax.experimental import pallas as pl
from jax.experimental.pallas import tpu as pltpu
from jax.sharding import PartitionSpec as P

HEAD_DIM = 128
PAIR = 2 * HEAD_DIM
PRIME = 32749
SIZES = (2, 3, 5, 6)
F32 = jnp.float32
BF16 = jnp.bfloat16
MESH = pl.DeviceIdType.MESH

NN = (((1,), (0,)), ((), ()))
NT = (((1,), (1,)), ((), ()))
TN = (((0,), (0,)), ((), ()))


def dot(left, right, dims=NN):
    return lax.dot_general(left, right, dims, preferred_element_type=F32)


def low(left, right, dims=NN):
    return dot(left.astype(BF16), right.astype(BF16), dims)


def halves(array):
    high = array.astype(BF16)
    return high, (array - high.astype(F32)).astype(BF16)


def modulo(whole):
    times = (whole.astype(F32) * (1.0 / PRIME)).astype(jnp.int32)
    left = whole - times * PRIME
    left = jnp.where(left < 0, left + PRIME, left)
    return jnp.where(left >= PRIME, left - PRIME, left)


def wrap(value):
    return jnp.where(value >= PRIME, value - PRIME, value)


def fill_pattern(pattern, first_col, between):
    step = 16
    width, feat = pattern.shape
    rows = lax.broadcasted_iota(jnp.int32, (step, 1), 0) * 1103 + 7
    cols = modulo((first_col + lax.broadcasted_iota(jnp.int32, (1, feat), 1)) * 2713)
    start = wrap(rows + cols)
    jump = step * 1103 % PRIME
    square = modulo(start * start).astype(F32)
    change = modulo(start * (2 * jump) + jump * jump).astype(F32)
    bend = float(2 * jump * jump % PRIME)
    round_to = float(3 << 22)

    def body(n, state):
        square, change = state
        tenth = square * 0.1 + 0.05
        whole = (tenth + round_to) - round_to
        signs = jnp.where(tenth >= whole, 1.0, -1.0)
        pattern[pl.ds(pl.multiple_of(n * step, step), step), :] = signs.astype(BF16)
        return wrap(square + change), wrap(change + bend)

    middle = width // step // 2
    state = lax.fori_loop(0, middle, body, (square, change), unroll=4)
    between()
    lax.fori_loop(middle, width // step, body, state, unroll=4)


def rotate(array, cos, sin):
    return array * cos + pltpu.roll(array, HEAD_DIM // 2, 1) * sin


def unrotate(array, cos, sin):
    return array * cos - pltpu.roll(array, HEAD_DIM // 2, 1) * sin


def kernel(
    groups,
    parts,
    entries,
    chunks,
    weights_hbm,
    seg_hbm,
    model_hbm,
    head_hbm,
    gain_hbm,
    cosine_hbm,
    sine_hbm,
    tokens_hbm,
    targets_hbm,
    wq_hbm,
    wk_hbm,
    wv_hbm,
    wo_hbm,
    diag_query,
    diag_key,
    mean_out,
    weights_row,
    seg_row,
    model_bits,
    head_bits,
    gain,
    cosine,
    sine,
    tokens,
    targets,
    wq,
    wk,
    wv,
    wo,
    wo_turned,
    normed,
    signed,
    slabs,
    slabs_turned,
    pattern,
    product,
    left_main,
    left_rest,
    right_main,
    right_rest,
    values,
    soft,
    d_soft,
    attended,
    out_send,
    own_part,
    pair_recv,
    chip_send,
    chip_recv,
    residual,
    hk_sum,
    gathered,
    x_send,
    x_recv,
    own_sum,
    result,
    stat_send,
    stat_recv,
    stat_all,
    load_sem,
    slab_ssem,
    slab_rsem,
    share_ssem,
    share_rsem,
    pair_ssem,
    pair_rsem,
    chip_ssem,
    chip_rsem,
    res_ssem,
    res_rsem,
    line_ssem,
    line_rsem,
    x_ssem,
    x_rsem,
    stat_ssem,
    stat_rsem,
    all_ssem,
    all_rsem,
    out_sem,
    small_sem,
):
    seq, width = tokens.shape
    feat = wq.shape[1]
    heads = feat // HEAD_DIM
    block = width // groups
    lines = groups // 2
    slab = 2 * block
    half = seq // 2
    count = len(chunks)
    dp = lax.axis_index("dp")
    mp = lax.axis_index("mp")
    kind = lax.rem(mp, 2)
    other = 1 - kind
    pair = mp + 1 - 2 * kind
    chip = lax.rem(mp + 2, parts)
    inner = lax.rem(dp, 2)
    outer = dp // 2
    x_peer = dp + 1 - 2 * inner

    loads = []
    for n, (source, target) in enumerate(
        (
            (tokens_hbm, tokens),
            (wq_hbm, wq),
            (wk_hbm, wk),
            (wv_hbm, wv),
            (wo_hbm, wo),
            (targets_hbm, targets),
        )
    ):
        loads.append(pltpu.make_async_copy(source, target, load_sem.at[n]))
    loads[0].start()
    smalls = []
    for n, (source, target) in enumerate(
        (
            (model_hbm, model_bits),
            (gain_hbm, gain),
            (head_hbm, head_bits),
            (cosine_hbm, cosine),
            (sine_hbm, sine),
            (seg_hbm, seg_row),
            (weights_hbm, weights_row),
        )
    ):
        small = pltpu.make_async_copy(source, target, small_sem.at[n])
        small.start()
        smalls.append(small)

    barrier = pltpu.get_barrier_semaphore()
    for step in range(1, lines):
        peer = lax.rem(outer + step, lines) * 2 + inner
        pl.semaphore_signal(barrier, inc=1, device_id={"dp": peer}, device_id_type=MESH)
    pl.semaphore_signal(barrier, inc=1, device_id={"dp": x_peer}, device_id_type=MESH)
    pl.semaphore_signal(barrier, inc=1, device_id={"mp": pair}, device_id_type=MESH)
    pl.semaphore_signal(barrier, inc=1, device_id={"mp": chip}, device_id_type=MESH)

    def load_more():
        loads[1].start()
        loads[2].start()

    fill_pattern(pattern, mp * feat, load_more)

    for small in smalls:
        small.wait()
    model_sign = 2.0 * model_bits[...].astype(F32) - 1.0
    head_sign = 2.0 * head_bits[0].astype(F32) - 1.0
    loads[0].wait()
    token_float = tokens[...].astype(F32)
    inverse = lax.rsqrt(jnp.sum(token_float * token_float, axis=1, keepdims=True) / width + 1e-06)
    for start in range(0, width, 256):
        cols = slice(start, start + 256)
        part = (tokens[:, cols].astype(F32) * inverse * gain[:, cols]).astype(BF16)
        normed[:, cols] = part
        signed[:, cols] = (part.astype(F32) * model_sign[:, cols]).astype(BF16)

    for load in loads[3:]:
        load.start()
    pl.semaphore_wait(barrier, lines + 2)

    def slab_copy(step):
        peer = lax.rem(outer + step, lines)
        return pltpu.make_async_remote_copy(
            src_ref=signed.at[
                pl.ds(pl.multiple_of(kind * half, half), half),
                pl.ds(pl.multiple_of(peer * slab, slab), slab),
            ],
            dst_ref=slabs.at[outer, pl.ds(pl.multiple_of(kind * half, half), half), :],
            send_sem=slab_ssem.at[step],
            recv_sem=slab_rsem.at[step],
            device_id={"dp": peer * 2 + inner},
            device_id_type=MESH,
        )

    def share_copy(step):
        owner = lax.rem(outer - step + lines, lines)
        mine = slabs.at[owner, pl.ds(pl.multiple_of(kind * half, half), half), :]
        return pltpu.make_async_remote_copy(
            src_ref=mine,
            dst_ref=mine,
            send_sem=share_ssem.at[step],
            recv_sem=share_rsem.at[step],
            device_id={"mp": pair},
            device_id_type=MESH,
        )

    for step in range(1, lines):
        slab_copy(step).start()

    cos = cosine[...]
    sin = sine[...]
    scale = HEAD_DIM ** (-0.5)

    product[...] = dot(signed[...], pattern[...])
    for h in range(heads):
        cols = slice(h * HEAD_DIM, (h + 1) * HEAD_DIM)
        probe = product[:, cols]
        high, rest = halves(rotate(probe * head_sign[0:1, cols], cos, sin))
        left_main[h, :, :HEAD_DIM] = high
        left_rest[h, :, :HEAD_DIM] = rest
        high, rest = halves(rotate(probe * head_sign[1:2, cols], cos, sin))
        right_main[h, :, HEAD_DIM:] = high
        right_rest[h, :, HEAD_DIM:] = rest
    loads[1].wait()
    query = dot(normed[...], wq[...])
    for h in range(heads):
        cols = slice(h * HEAD_DIM, (h + 1) * HEAD_DIM)
        high, rest = halves(rotate(query[:, cols], cos, sin))
        left_main[h, :, HEAD_DIM:] = high
        left_rest[h, :, HEAD_DIM:] = rest
    loads[2].wait()
    keys = dot(normed[...], wk[...])
    for h in range(heads):
        cols = slice(h * HEAD_DIM, (h + 1) * HEAD_DIM)
        high, rest = halves(rotate(keys[:, cols], cos, sin))
        right_main[h, :, :HEAD_DIM] = high
        right_rest[h, :, :HEAD_DIM] = rest
    loads[3].wait()
    values[...] = dot(normed[...], wv[...]).astype(BF16)

    place_q = lax.broadcasted_iota(jnp.int32, (seq, seq), 0)
    place_k = lax.broadcasted_iota(jnp.int32, (seq, seq), 1)
    same = place_q == place_k
    segments = seg_row[...].astype(F32)
    seg_col = jnp.sum(jnp.where(same, segments, 0.0), axis=1, keepdims=True)
    row_weights = jnp.sum(jnp.where(same, weights_row[...], 0.0), axis=1, keepdims=True) / seq

    def pair_copy(c):
        first, rows = chunks[c]
        return pltpu.make_async_remote_copy(
            src_ref=out_send.at[pl.ds(first, rows), :],
            dst_ref=pair_recv.at[pl.ds(first, rows), :],
            send_sem=pair_ssem.at[c],
            recv_sem=pair_rsem.at[c],
            device_id={"mp": pair},
            device_id_type=MESH,
        )

    def chip_copy(c):
        first, rows = chunks[c]
        return pltpu.make_async_remote_copy(
            src_ref=chip_send.at[pl.ds(first, rows), :],
            dst_ref=chip_recv.at[pl.ds(first, rows), :],
            send_sem=chip_ssem.at[c],
            recv_sem=chip_rsem.at[c],
            device_id={"mp": chip},
            device_id_type=MESH,
        )

    def res_copy(c, which):
        first, rows = chunks[c]
        return pltpu.make_async_remote_copy(
            src_ref=residual.at[which, pl.ds(first, rows), :],
            dst_ref=residual.at[which, pl.ds(first, rows), :],
            send_sem=res_ssem.at[c],
            recv_sem=res_rsem.at[c],
            device_id={"mp": pair},
            device_id_type=MESH,
        )

    def attend(c):
        first, rows = chunks[c]
        reach = first + rows
        span = slice(first, reach)
        place = first + lax.broadcasted_iota(jnp.int32, (rows, reach), 0)
        place = jnp.concatenate([place] * heads, axis=0)
        owner = jnp.concatenate([seg_col[span, :]] * heads, axis=0)
        allowed = (place >= lax.broadcasted_iota(jnp.int32, (heads * rows, reach), 1)) & (
            owner == segments[:, :reach]
        )
        blank = jnp.zeros((rows, HEAD_DIM), BF16)
        scores, d_scores = [], []
        for h in range(heads):
            both = left_main[h, span, :]
            rest = left_rest[h, span, :]
            q = jnp.concatenate([both[:, HEAD_DIM:], blank], axis=1)
            q_rest = jnp.concatenate([rest[:, HEAD_DIM:], blank], axis=1)
            main = dot(jnp.concatenate([both, rest, q, q_rest], axis=0), right_main[h, :reach, :], NT)
            minor = dot(jnp.concatenate([both, q], axis=0), right_rest[h, :reach, :], NT)
            d_scores.append(main[:rows] + (main[rows : 2 * rows] + minor[:rows]))
            scores.append(main[2 * rows : 3 * rows] + (main[3 * rows :] + minor[rows:]))
        scores = jnp.concatenate(scores, axis=0) * scale
        d_scores = jnp.concatenate(d_scores, axis=0) * scale
        raised = jnp.where(allowed, jnp.exp(scores), 0.0)
        p = raised / jnp.sum(raised, axis=1, keepdims=True)
        d_p = p * (d_scores - jnp.sum(p * d_scores, axis=1, keepdims=True))
        soft[:, span, :reach] = p.reshape(heads, rows, reach)
        d_soft[:, span, :reach] = d_p.reshape(heads, rows, reach)
        p = p.astype(BF16)
        d_p = d_p.astype(BF16)
        for h in range(heads):
            cols = slice(h * HEAD_DIM, (h + 1) * HEAD_DIM)
            own = slice(h * rows, (h + 1) * rows)
            mixed = dot(jnp.concatenate([p[own], d_p[own]], axis=0), values[:reach, cols]).astype(BF16)
            attended[0, span, cols] = mixed[:rows]
            attended[1, span, cols] = mixed[rows:]

    def project(c):
        first, rows = chunks[c]
        span = slice(first, first + rows)
        out_send[span, :] = dot(attended[other, span, :], wo[...]).astype(BF16)
        pair_copy(c).start()
        own_part[span, :] = dot(attended[kind, span, :], wo[...])

    def forward(c):
        first, rows = chunks[c]
        span = slice(first, first + rows)
        pair_copy(c).wait_recv()
        summed = own_part[span, :] + pair_recv[span, :].astype(F32)
        own_part[span, :] = summed
        chip_send[span, :] = summed.astype(BF16)
        chip_copy(c).start()

    def line_copy(c, h, slot, target, way):
        first, rows = chunks[c]
        here = gathered.at[h, slot, pl.ds(first, rows), :]
        return pltpu.make_async_remote_copy(
            src_ref=here,
            dst_ref=here,
            send_sem=line_ssem.at[c, h, way],
            recv_sem=line_rsem.at[c, h, slot],
            device_id={"dp": target * 2 + inner},
            device_id_type=MESH,
        )

    def line_wait(c, h, slot):
        line_copy(c, h, slot, outer, 0).wait_recv()

    def own_sends(c, h, act, near=True, far=True):
        for way, hop in enumerate((2, -2, 1, -1)):
            if not (near if abs(hop) == 1 else far):
                continue

            @pl.when((outer + hop >= 0) & (outer + hop < lines))
            def _():
                act(line_copy(c, h, outer, outer + hop, way))

    def relays(c, h, step, side, act, arrive):
        slot = outer - side * 2 * step
        for n in range(2):
            hop = side * (n + 1)

            @pl.when((slot >= 0) & (slot < lines) & (outer + hop >= 0) & (outer + hop < lines))
            def _():
                if arrive and n == 0:
                    line_wait(c, h, slot)
                act(line_copy(c, h, slot, outer + hop, 4 * step + (side + 1) + n))

    def relay(c, h):
        for step in range(1, (lines + 1) // 2):
            for side in (1, -1):
                relays(c, h, step, side, lambda copy: copy.start(), True)

    def arrive(c, h):
        for slot in range(lines):
            gap = outer - slot
            far = jnp.abs(gap)
            onward = jnp.where(gap > 0, outer + 1 < lines, outer >= 1)
            passed = (lax.rem(far, 2) == 0) & onward

            @pl.when((far > 0) & jnp.logical_not(passed))
            def _():
                line_wait(c, h, slot)

    wanted = jnp.where(kind == 0, 1.0, 0.0)
    sums = [jnp.zeros((1, HEAD_DIM), F32), jnp.zeros((1, HEAD_DIM), F32)]

    def curve(c):
        first, rows = chunks[c]
        reach = first + rows
        span = slice(first, reach)
        chip_copy(c).wait_recv()
        whole = own_part[span, :] + chip_recv[span, :].astype(F32)
        shift = tokens[span, :].astype(F32) - targets[span, :].astype(F32)
        residual[kind, span, :] = ((whole + wanted * shift) * row_weights[span, :]).astype(BF16)
        res_copy(c, kind).start()
        back_own = dot(residual[kind, span, :], wo_turned[...])
        res_copy(c, other).wait_recv()
        back_other = dot(residual[other, span, :], wo_turned[...])
        back = jnp.where(kind == 0, back_own, back_other).astype(BF16)
        back_tangent = jnp.where(kind == 0, back_other, back_own).astype(BF16)
        cos_q = cos[span, :]
        sin_q = sin[span, :]
        u, u_tangent = [], []
        for h in range(heads):
            cols = slice(h * HEAD_DIM, (h + 1) * HEAD_DIM)
            pulled = dot(
                jnp.concatenate([back[:, cols], back_tangent[:, cols]], axis=0), values[:reach, cols], NT
            )
            u.append(pulled[:rows])
            u_tangent.append(pulled[rows:])
        u = jnp.concatenate(u, axis=0)
        u_tangent = jnp.concatenate(u_tangent, axis=0)
        p = soft[:, span, :reach].reshape(heads * rows, reach)
        d_p = d_soft[:, span, :reach].reshape(heads * rows, reach)
        centered = u - jnp.sum(p * u, axis=1, keepdims=True)
        level = jnp.sum(d_p * u + p * u_tangent, axis=1, keepdims=True)
        all_mixed = ((d_p * centered + p * (u_tangent - level)) * scale).astype(BF16)
        all_lead = (p * centered * scale).astype(BF16)
        for h in range(heads):
            cols = slice(h * HEAD_DIM, (h + 1) * HEAD_DIM)
            left = left_main[h, span, :]
            right = right_main[h, :reach, :]
            mixed = all_mixed[h * rows : (h + 1) * rows]
            lead = all_lead[h * rows : (h + 1) * rows]
            hq = dot(mixed, right[:, :HEAD_DIM]) + dot(lead, right[:, HEAD_DIM:])
            hk = dot(
                jnp.concatenate([mixed, lead], axis=0),
                jnp.concatenate([left[:, HEAD_DIM:], left[:, :HEAD_DIM]], axis=0),
                TN,
            )
            if c > 0:
                hk = hk_sum[:reach, cols] + hk
            if c < count - 1:
                hk_sum[:reach, cols] = hk
            hq = unrotate(hq, cos_q, sin_q)
            hk = unrotate(hk[span, :], cos_q, sin_q)
            hq = (hq.astype(BF16).astype(F32) * head_sign[0:1, cols]).astype(BF16)
            hk = (hk.astype(BF16).astype(F32) * head_sign[1:2, cols]).astype(BF16)
            gathered[h, outer, span, :HEAD_DIM] = hq
            gathered[h, outer, span, HEAD_DIM:] = hk
            own_sends(c, h, lambda copy: copy.start(), near=c < count - 1)
            probe = product[span, cols]
            sums[0] = sums[0] + jnp.sum(hq.astype(F32) * probe, axis=0, keepdims=True)
            sums[1] = sums[1] + jnp.sum(hk.astype(F32) * probe, axis=0, keepdims=True)

    def gather_slabs():
        for step in range(1, lines):
            slab_copy(step).wait_recv()
            share_copy(step).start()
        slabs[outer] = signed[:, pl.ds(pl.multiple_of(outer * slab, slab), slab)]

    def turn_slabs():
        for step in range(1, lines):
            share_copy(step).wait_recv()
        for o in range(lines):
            slabs_turned[:, o * seq : (o + 1) * seq] = jnp.transpose(slabs[o])

    attend(0)
    loads[4].wait()
    project(0)
    forward(0)
    for c in (1, 2):
        attend(c)
        project(c)
        forward(c)
    loads[5].wait()
    wo_turned[...] = jnp.transpose(wo[...])
    curve(0)
    for c in range(3, count):
        attend(c)
        project(c)
        forward(c)
    gather_slabs()
    curve(1)
    for h in range(heads):
        relay(0, h)
    turn_slabs()
    for c in range(2, count):
        curve(c)
        for h in range(heads):
            relay(c - 1, h)

    lane = lax.broadcasted_iota(jnp.int32, (1, HEAD_DIM), 1)
    stat_send[0] = jnp.where(
        lane < HEAD_DIM // 2,
        jnp.sum(sums[0], axis=1, keepdims=True),
        jnp.sum(sums[1], axis=1, keepdims=True),
    )

    def stat_copy(n):
        target = ({"mp": pair}, {"mp": chip}, {"dp": x_peer})[n]
        return pltpu.make_async_remote_copy(
            src_ref=stat_send.at[n],
            dst_ref=stat_recv.at[n],
            send_sem=stat_ssem.at[n],
            recv_sem=stat_rsem.at[n],
            device_id=target,
            device_id_type=MESH,
        )

    def all_copy(step):
        return pltpu.make_async_remote_copy(
            src_ref=stat_all.at[outer],
            dst_ref=stat_all.at[outer],
            send_sem=all_ssem.at[step],
            recv_sem=all_rsem.at[step],
            device_id={"dp": lax.rem(outer + step, lines) * 2 + inner},
            device_id_type=MESH,
        )

    def x_copy(h):
        return pltpu.make_async_remote_copy(
            src_ref=x_send.at[h],
            dst_ref=x_recv.at[h],
            send_sem=x_ssem.at[h],
            recv_sem=x_rsem.at[h],
            device_id={"dp": x_peer},
            device_id_type=MESH,
        )

    stat_copy(0).start()
    own_rows = pl.ds(pl.multiple_of(inner * block, block), block)
    peer_rows = pl.ds(pl.multiple_of((1 - inner) * block, block), block)
    for h in range(heads):
        own_sends(count - 1, h, lambda copy: copy.start(), far=False)
        relay(count - 1, h)
        if h < 3:
            stat_copy(h).wait_recv()
            total = stat_send[h] + stat_recv[h]
            if h < 2:
                stat_send[h + 1] = total
                stat_copy(h + 1).start()
            else:
                stat_all[outer] = total
                for step in range(1, lines):
                    all_copy(step).start()
    for h in range(heads):
        for c in range(count):
            arrive(c, h)
        stack = gathered[h].reshape(lines * seq, PAIR)
        x_send[h] = dot(slabs_turned[peer_rows, :], stack).astype(BF16)
        x_copy(h).start()
        own_sum[h] = dot(slabs_turned[own_rows, :], stack)

    def out_copies(h):
        cols = pl.ds(h * HEAD_DIM, HEAD_DIM)
        return [
            pltpu.make_async_copy(result.at[n, :, cols], target.at[:, cols], out_sem.at[n, h])
            for n, target in enumerate((diag_query, diag_key))
        ]

    for h in range(heads):
        cols = slice(h * HEAD_DIM, (h + 1) * HEAD_DIM)
        signs = pattern[pl.ds(pl.multiple_of(dp * block, block), block), cols].astype(F32) * (1.0 / groups)
        x_copy(h).wait_recv()
        total = own_sum[h] + x_recv[h].astype(F32)
        result[0, :, cols] = total[:, :HEAD_DIM] * signs
        result[1, :, cols] = total[:, HEAD_DIM:] * signs
        for copy in out_copies(h):
            copy.start()
    for step in range(1, lines):
        all_copy(step).wait_recv()
    mean_out[...] = jnp.sum(stat_all[...], axis=0) * (1.0 / groups) / entries

    for step in range(1, lines):
        slab_copy(step).wait_send()
        share_copy(step).wait_send()
        all_copy(step).wait_send()
    for c in range(count):
        pair_copy(c).wait_send()
        chip_copy(c).wait_send()
        res_copy(c, kind).wait_send()
        for h in range(heads):
            own_sends(c, h, lambda copy: copy.wait_send())
            for step in range(1, (lines + 1) // 2):
                for side in (1, -1):
                    relays(c, h, step, side, lambda copy: copy.wait_send(), False)
    for n in range(3):
        stat_copy(n).wait_send()
    for h in range(heads):
        x_copy(h).wait_send()
        for copy in out_copies(h):
            copy.wait()


def finish(query_in, key_in, mean_in, query_out, key_out, mean_out, held, sem):
    rows = query_in.shape[0] // 2
    moves = []
    for n, (source, target) in enumerate(((query_in, query_out), (key_in, key_out))):
        for part in range(2):
            span = pl.ds(part * rows, rows)
            slot = held.at[n, span, :]
            take = pltpu.make_async_copy(source.at[span, :], slot, sem.at[0, n, part])
            give = pltpu.make_async_copy(slot, target.at[span, :], sem.at[1, n, part])
            take.start()
            moves.append((take, give))
    mean_out[0] = mean_in[0, 0]
    mean_out[1] = mean_in[0, HEAD_DIM // 2]
    for take, give in moves:
        take.wait()
        give.start()
    for take, give in moves:
        give.wait()


def local(
    tokens,
    targets,
    loss_weights,
    segments,
    probe_model,
    probe_heads,
    norm_gain,
    w_query,
    w_key,
    w_value,
    w_out,
):
    groups = lax.axis_size("dp")
    parts = lax.axis_size("mp")
    assert parts == 4 and groups % 2 == 0
    seq, width = tokens.shape
    feat = w_query.shape[1]
    heads = feat // HEAD_DIM
    block = width // groups
    lines = groups // 2
    sizes = [part * seq // 16 for part in SIZES]
    chunks = tuple((seq - sum(sizes[: n + 1]), size) for n, size in enumerate(sizes))
    count = len(chunks)
    position = np.arange(seq, dtype=np.float32)
    exponent = np.arange(0, HEAD_DIM, 2).astype(np.float32) / np.float32(HEAD_DIM)
    angles = position[:, None] * (np.float32(10000.0) ** (-exponent)).astype(np.float32)[None, :]
    cos = np.cos(angles.astype(np.float64)).astype(np.float32)
    sin = np.sin(angles.astype(np.float64)).astype(np.float32)
    cosine = np.concatenate([cos, cos], axis=1)
    sine = np.concatenate([-sin, sin], axis=1)
    vmem = pl.BlockSpec(memory_space=pltpu.VMEM)
    anywhere = pl.BlockSpec(memory_space=pl.ANY)
    dma = pltpu.SemaphoreType.DMA
    ways = 4 + 4 * ((lines + 1) // 2 - 1) + 4
    diag_query, diag_key, means = pl.pallas_call(
        functools.partial(kernel, groups, parts, float(width * feat * parts), chunks),
        out_shape=(
            jax.ShapeDtypeStruct((block, feat), F32),
            jax.ShapeDtypeStruct((block, feat), F32),
            jax.ShapeDtypeStruct((1, HEAD_DIM), F32),
        ),
        in_specs=[pl.BlockSpec(memory_space=pltpu.HBM)] * 13,
        out_specs=(anywhere, anywhere, vmem),
        scratch_shapes=[
            pltpu.VMEM((1, seq), F32),
            pltpu.VMEM((1, seq), jnp.int32),
            pltpu.VMEM((1, width), jnp.int32),
            pltpu.VMEM((1, 2, feat), jnp.int32),
            pltpu.VMEM((1, width), F32),
            pltpu.VMEM((seq, HEAD_DIM), F32),
            pltpu.VMEM((seq, HEAD_DIM), F32),
            pltpu.VMEM((seq, width), BF16),
            pltpu.VMEM((seq, width), BF16),
            pltpu.VMEM((width, feat), BF16),
            pltpu.VMEM((width, feat), BF16),
            pltpu.VMEM((width, feat), BF16),
            pltpu.VMEM((feat, width), BF16),
            pltpu.VMEM((width, feat), BF16),
            pltpu.VMEM((seq, width), BF16),
            pltpu.VMEM((seq, width), BF16),
            pltpu.VMEM((lines, seq, 2 * block), BF16),
            pltpu.VMEM((2 * block, lines * seq), BF16),
            pltpu.VMEM((width, feat), BF16),
            pltpu.VMEM((seq, feat), F32),
            pltpu.VMEM((heads, seq, PAIR), BF16),
            pltpu.VMEM((heads, seq, PAIR), BF16),
            pltpu.VMEM((heads, seq, PAIR), BF16),
            pltpu.VMEM((heads, seq, PAIR), BF16),
            pltpu.VMEM((seq, feat), BF16),
            pltpu.VMEM((heads, seq, seq), F32),
            pltpu.VMEM((heads, seq, seq), F32),
            pltpu.VMEM((2, seq, feat), BF16),
            pltpu.VMEM((seq, width), BF16),
            pltpu.VMEM((seq, width), F32),
            pltpu.VMEM((seq, width), BF16),
            pltpu.VMEM((seq, width), BF16),
            pltpu.VMEM((seq, width), BF16),
            pltpu.VMEM((2, seq, width), BF16),
            pltpu.VMEM((seq, feat), F32),
            pltpu.VMEM((heads, lines, seq, PAIR), BF16),
            pltpu.VMEM((heads, block, PAIR), BF16),
            pltpu.VMEM((heads, block, PAIR), BF16),
            pltpu.VMEM((heads, block, PAIR), F32),
            pltpu.VMEM((2, block, feat), F32),
            pltpu.VMEM((3, 1, HEAD_DIM), F32),
            pltpu.VMEM((3, 1, HEAD_DIM), F32),
            pltpu.VMEM((lines, 1, HEAD_DIM), F32),
            dma((6,)),
            dma((lines,)),
            dma((lines,)),
            dma((lines,)),
            dma((lines,)),
            dma((count,)),
            dma((count,)),
            dma((count,)),
            dma((count,)),
            dma((count,)),
            dma((count,)),
            dma((count, heads, ways)),
            dma((count, heads, lines)),
            dma((heads,)),
            dma((heads,)),
            dma((3,)),
            dma((3,)),
            dma((lines,)),
            dma((lines,)),
            dma((2, heads)),
            dma((7,)),
        ],
        compiler_params=pltpu.CompilerParams(
            collective_id=0, has_side_effects=True, vmem_limit_bytes=62 * 1024 * 1024
        ),
    )(
        loss_weights.reshape(1, seq),
        segments,
        probe_model,
        probe_heads,
        norm_gain.reshape(1, width),
        jnp.asarray(cosine),
        jnp.asarray(sine),
        tokens,
        targets,
        w_query,
        w_key,
        w_value,
        w_out,
    )
    return pl.pallas_call(
        finish,
        out_shape=(
            jax.ShapeDtypeStruct((block, feat), F32),
            jax.ShapeDtypeStruct((block, feat), F32),
            jax.ShapeDtypeStruct((2,), F32),
        ),
        in_specs=[anywhere, anywhere, pl.BlockSpec(memory_space=pltpu.SMEM)],
        out_specs=(anywhere, anywhere, pl.BlockSpec(memory_space=pltpu.SMEM)),
        scratch_shapes=[pltpu.VMEM((2, block, feat), F32), dma((2, 2, 2))],
    )(diag_query, diag_key, means)


def solution(mesh):
    placed = (
        P("dp", None),
        P("dp", None),
        P("dp"),
        P("dp", None),
        P("dp", None),
        P("dp", None, "mp"),
        P(),
        P(None, "mp"),
        P(None, "mp"),
        P(None, "mp"),
        P("mp", None),
    )
    return jax.shard_map(
        local,
        mesh=mesh,
        in_specs=placed,
        out_specs=(P("dp", "mp"), P("dp", "mp"), P()),
        check_vma=False,
    )
```
